8 devices in a mesh: dp: 1 (over z), sp: 8 (over x, y, core).
Axes of the slice: x: 2, y: 2, z: 1, core: 2. Of those that a mesh axis runs over, the one named last changes fastest.
Arguments:
- x: bfloat16 [4096, 2048], P(('dp', 'sp'))
- gain: bfloat16 [2048], replicated
- wq: bfloat16 [2048, 4096], replicated
- wk: bfloat16 [2048, 2048], replicated
- wv: bfloat16 [2048, 2048], replicated
- wo: bfloat16 [4096, 2048], replicated
Outputs:
- output: bfloat16 [4096, 2048], P(('dp', 'sp'))
All inputs are finite; a program needn't handle non-finite values.
Results may differ from the reference program's by a relative error of at most 0.012.
Values are sent between devices in bfloat16 or wider.
A program may use at most 2 GiB of HBM per device.

```python
import jax
import jax.numpy as jnp
from jax import lax

ROWS = 4096
D = 2048
HEADS = 32
KV_HEADS = 16
HEAD = 128
THETA = 10000


def setup_inputs(seed: int = 0, part: int = 0) -> dict:
    kx, kn, kq, kk, kv, ko = jax.random.split(jax.random.key(seed), 6)

    def weights(key, rows, columns):
        return jax.random.normal(key, (rows, columns), jnp.float32) * rows**-0.5

    drawn = {
        "x": jax.random.normal(jax.random.fold_in(kx, part), (ROWS, D), jnp.float32),
        "gain": 1 + 0.1 * jax.random.normal(kn, (D,), jnp.float32),
        "wq": 2 * weights(kq, D, HEADS * HEAD),
        "wk": 2 * weights(kk, D, KV_HEADS * HEAD),
        "wv": 4 * weights(kv, D, KV_HEADS * HEAD),
        "wo": weights(ko, HEADS * HEAD, D),
    }
    return {k: v.astype(jnp.bfloat16) for k, v in drawn.items()}


def normed(x, gain):
    wide = x.astype(jnp.float32)
    scale = lax.rsqrt(jnp.mean(wide * wide, -1, keepdims=True) + 1e-6)
    return (wide * scale * gain.astype(jnp.float32)).astype(jnp.bfloat16)


def turned(t, place, theta):
    half = t.shape[-1] // 2
    angle = place.astype(jnp.float32)[:, None] * theta ** (-jnp.arange(half, dtype=jnp.float32) / half)
    cos, sin = jnp.cos(angle)[:, None], jnp.sin(angle)[:, None]
    a, b = t[..., :half].astype(jnp.float32), t[..., half:].astype(jnp.float32)
    return jnp.concatenate([a * cos - b * sin, b * cos + a * sin], -1).astype(jnp.bfloat16)


def matmul(a, w):
    return jnp.dot(a, w, preferred_element_type=jnp.float32).astype(jnp.bfloat16)


def einsum(form, a, b):
    return jnp.einsum(form, a.astype(jnp.float32), b.astype(jnp.float32))


def attention(q, k, v):
    scores = einsum("tgsd,ugd->gstu", q, k) * q.shape[-1] ** -0.5
    token = jnp.arange(q.shape[0])
    scores = jnp.where(token[:, None] >= token, scores, -jnp.inf)
    weights = jax.nn.softmax(scores, -1).astype(jnp.bfloat16)
    return einsum("gstu,ugd->tgsd", weights, v).astype(jnp.bfloat16)


def reference(x, gain, wq, wk, wv, wo):
    a, place = normed(x, gain), jnp.arange(ROWS)
    q = turned(matmul(a, wq).reshape(ROWS, HEADS, HEAD), place, THETA).reshape(ROWS, KV_HEADS, -1, HEAD)
    k = turned(matmul(a, wk).reshape(ROWS, KV_HEADS, HEAD), place, THETA)
    v = matmul(a, wv).reshape(ROWS, KV_HEADS, HEAD)
    seen = attention(q, k, v).reshape(ROWS, HEADS * HEAD)
    return (x.astype(jnp.float32) + jnp.dot(seen, wo, preferred_element_type=jnp.float32)).astype(jnp.bfloat16)
```

```python
import functools

import jax
import jax.numpy as jnp
import numpy as np
from jax import lax
from jax.experimental import pallas as pl
from jax.experimental.pallas import tpu as pltpu
from jax.sharding import PartitionSpec as P

MESH = pl.DeviceIdType.MESH
NEG = -1e30
HIDDEN = 2 * NEG
LOG2E = 1.4426950408889634
HEAD = 128
THETA = 10000
N = 8
BLK = 512
HALF = BLK // 2
QUARTER = BLK // 4
DM = 2048
QW = 512
KW = 256
ROWS_V = 144


def _dot(a, b, ca, cb):
    return lax.dot_general(a, b, (((ca,), (cb,)), ((), ())), preferred_element_type=jnp.float32)


def _xor(a, b):
    bit = lambda v, w: lax.rem(lax.div(v, w), 2)
    return sum(lax.rem(bit(a, w) + bit(b, w), 2) * w for w in (4, 2, 1))


def _mega(a_hbm, wq_hbm, wk_hbm, wv_hbm, loc_ref, base_ref, o_hbm,
          abuf, w, q, k, vt, acc, top, ob,
          loc_sem, w_sem, dsem, sibsem, qasem, qbsem, s_sib, s_dir, s_rel, s_fwd, s_o, osem, oloc):
    i32 = lambda v: jnp.asarray(v, jnp.int32)
    d = lax.axis_index("sp").astype(jnp.int32)
    z = lax.rem(d, 2)
    nz = 1 - z
    sib, ynb, xnb = (_xor(d, i32(m)) for m in (1, 2, 4))
    e = HEAD**-0.5 * LOG2E

    own = pltpu.make_async_copy(a_hbm, abuf.at[0], loc_sem)
    own.start()
    loads = [
        pltpu.make_async_copy(wq_hbm.at[:, pl.ds(pl.multiple_of(d * QW, QW), QW)], w.at[:, 0:QW], w_sem.at[0]),
        pltpu.make_async_copy(wk_hbm.at[:, pl.ds(pl.multiple_of(d * KW, KW), KW)], w.at[:, QW : QW + KW], w_sem.at[1]),
        pltpu.make_async_copy(wv_hbm.at[:, pl.ds(pl.multiple_of(d * KW, KW), KW)], w.at[:, QW + KW : QW + 2 * KW], w_sem.at[2]),
    ]
    for c in loads:
        c.start()
    barrier = pltpu.get_barrier_semaphore()
    for m in range(1, N):
        pl.semaphore_signal(barrier, inc=1, device_id={"sp": _xor(d, i32(m))}, device_id_type=MESH)
    pl.semaphore_wait(barrier, N - 1)

    def part(src, dst, at, rows, dev, ssem, rsem):
        here = pl.ds(pl.multiple_of(at, QUARTER), rows)
        return pltpu.make_async_remote_copy(abuf.at[src, here], abuf.at[dst, here], ssem, rsem, device_id={"sp": dev}, device_id_type=MESH)

    sib_a = part(0, 1, nz * HALF, HALF, sib, s_sib.at[0], dsem.at[1])
    sib_b = part(0, 1, z * HALF, HALF, sib, s_sib.at[1], sibsem.at[1])

    def to_y(zz):
        return part(_xor1(zz), 2 + _xor1(zz), z * HALF, HALF, ynb, s_dir.at[zz, 0], dsem.at[2 + _xor1(zz)])

    def to_x(zz):
        return part(_xor1(zz), 4 + _xor1(zz), z * HALF, HALF, xnb, s_dir.at[zz, 1], dsem.at[4 + _xor1(zz)])

    def _xor1(zz):
        return lax.rem(zz + z, 2)

    def relay_x(zz):
        return part(2 + _xor1(zz), 6 + _xor1(zz), z * HALF, QUARTER, xnb, s_rel.at[zz, 0], qasem.at[_xor1(zz)])

    def relay_y(zz):
        return part(4 + _xor1(zz), 6 + _xor1(zz), z * HALF + QUARTER, QUARTER, ynb, s_rel.at[zz, 1], qbsem.at[_xor1(zz)])

    def forward(p):
        return part(p, _xor(p, i32(1)), z * HALF, HALF, sib, s_fwd.at[p], sibsem.at[_xor(p, i32(1))])

    own.wait()
    sib_a.start()

    @pl.when(z == 0)
    def _():
        to_y(i32(0)).start()
        to_x(i32(0)).start()

    sib_b.start()
    sib_a.wait_recv()

    @pl.when(z == 1)
    def _():
        to_y(i32(0)).start()
        to_x(i32(0)).start()

    to_y(i32(1)).start()
    to_x(i32(1)).start()
    for c in loads:
        c.wait()

    ones = jnp.ones((ROWS_V - HEAD, BLK), jnp.bfloat16)
    lane = lax.broadcasted_iota(jnp.int32, (BLK, HEAD), 1)

    def project(p):
        s = _xor(d, p)
        cb, sb = base_ref[pl.ds(s, 1), :], base_ref[pl.ds(N + s, 1), :]
        cl, sl = loc_ref[0], loc_ref[1]
        cos = cb * cl - sb * sl
        sin = sb * cl + cb * sl
        sin = jnp.where(lane < HEAD // 2, -sin, sin)
        for c in range(4):
            y = _dot(abuf[p], w[:, c * 256 : (c + 1) * 256], 1, 0)
            for n in range(2):
                t = y[:, n * HEAD : (n + 1) * HEAD]
                if c < 3:
                    t = t.astype(jnp.bfloat16).astype(jnp.float32)
                    t = (t * cos + pltpu.roll(t, HEAD // 2, 1) * sin).astype(jnp.bfloat16)
                if c < 2:
                    q[p, c, n * BLK : (n + 1) * BLK, :] = t
                elif c == 2:
                    k[p, n] = t
                else:
                    vt[p, n, :HEAD, :] = t.T.astype(jnp.bfloat16)
                    vt[p, n, HEAD:, :] = ones
        top[p] = jnp.full((2, 1, 2 * BLK), NEG, jnp.float32)
        acc[p] = jnp.zeros((2, ROWS_V, 2 * BLK), jnp.float32)

    pieces = [(h, n * BLK) for h in range(2) for n in range(2)]

    def attend(pi, pj, masked):
        scores = [_dot(k[pj, h], q[pi, h, at : at + BLK, :], 1, 1) for h, at in pieces]
        if masked:
            ok = lax.broadcasted_iota(jnp.int32, (BLK, BLK), 1) >= lax.broadcasted_iota(jnp.int32, (BLK, BLK), 0)
        weights, keeps = [], []
        for (h, at), s in zip(pieces, scores):
            if masked:
                s = jnp.where(ok, s, HIDDEN)
            old = top[pi, h, :, at : at + BLK]
            new = jnp.maximum(old, s.max(axis=0, keepdims=True))
            top[pi, h, :, at : at + BLK] = new
            weights.append(jnp.exp2((s - new) * e).astype(jnp.bfloat16))
            keeps.append(jnp.exp2((old - new) * e))
        for (h, at), x, keep in zip(pieces, weights, keeps):
            acc[pi, h, :, at : at + BLK] = acc[pi, h, :, at : at + BLK] * keep + _dot(vt[pj, h], x, 1, 0)

    def group_of(p):
        r = lax.div(p, 2)
        return jnp.where(r == 0, 0, jnp.where(r == 3, 3, 1 + _xor1(lax.rem(p, 2))))

    def slot_of(g, u):
        return jnp.where(g == 0, u, jnp.where(g == 3, 6 + _xor1(u), 2 + 2 * u + _xor1(jnp.maximum(g - 1, 0))))

    def last_group(i):
        out = i32(0)
        for j in range(N):
            out = jnp.maximum(out, jnp.where(i32(j) <= i, group_of(_xor(d, i32(j))), 0))
        return out

    def result_copy(p):
        s = _xor(d, p)
        at = pl.ds(pl.multiple_of(d * QW, QW), QW)
        return pltpu.make_async_remote_copy(ob.at[p], o_hbm.at[:, at], s_o.at[p], osem.at[p], device_id={"sp": s}, device_id_type=MESH)

    def result_own():
        at = pl.ds(pl.multiple_of(d * QW, QW), QW)
        return pltpu.make_async_copy(ob.at[0], o_hbm.at[:, at], oloc)

    def finish(p, g):
        @pl.when(last_group(_xor(d, p)) == g)
        def _():
            for h in range(2):
                for n in range(2):
                    cols = slice(n * BLK, (n + 1) * BLK)
                    total = acc[p, h, HEAD : HEAD + 1, cols]
                    o = (acc[p, h, :HEAD, cols] * (1 / total)).T
                    ob[p, :, (2 * h + n) * HEAD : (2 * h + n + 1) * HEAD] = o.astype(jnp.bfloat16)

            @pl.when(p == 0)
            def _():
                result_own().start()

            @pl.when(p != 0)
            def _():
                result_copy(p).start()

    def group(g, _):
        @pl.when((g == 1) | (g == 2))
        def _():
            zz = g - 1
            ps, px = 2 + _xor1(zz), 4 + _xor1(zz)
            to_y(zz).wait_recv()
            relay_x(zz).start()
            forward(ps).start()
            to_x(zz).wait_recv()
            relay_y(zz).start()
            forward(px).start()

        def arrive(u, _):
            p = slot_of(g, u)

            @pl.when(g == 3)
            def _():
                relay_x(u).wait_recv()
                relay_y(u).wait_recv()
                forward(p).start()

            @pl.when(p != 0)
            def _():
                part(0, p, nz * HALF, HALF, sib, s_sib.at[0], sibsem.at[p]).wait_recv()

            project(p)
            return _

        lax.fori_loop(0, 2, arrive, None)
        p0, p1 = slot_of(g, i32(0)), slot_of(g, i32(1))
        b0, b1 = _xor(d, p0), _xor(d, p1)
        hi, lo = jnp.where(b0 > b1, p0, p1), jnp.where(b0 > b1, p1, p0)

        def pair(x, _):
            t, u = lax.div(x, 2), lax.rem(x, 2)
            told = slot_of(lax.div(t, 2), lax.rem(t, 2))
            new = jnp.where(u == 0, p0, p1)
            inner = t == 2 * g
            pa, pb = jnp.where(inner, hi, told), jnp.where(inner, lo, new)
            ba, bb = _xor(d, pa), _xor(d, pb)
            attend(jnp.where(ba > bb, pa, pb), jnp.where(ba > bb, pb, pa), False)

            @pl.when(u == 1)
            def _():
                finish(told, g)

            return _

        lax.fori_loop(0, 4 * g + 1, pair, None)

        def diagonal(u, _):
            p = jnp.where(u == 0, p0, p1)
            attend(p, p, True)
            finish(p, g)
            return _

        lax.fori_loop(0, 2, diagonal, None)
        return _

    lax.fori_loop(0, 4, group, None)

    sib_a.wait_send()
    sib_b.wait_send()
    for zz in range(2):
        to_y(i32(zz)).wait_send()
        to_x(i32(zz)).wait_send()
        relay_x(i32(zz)).wait_send()
        relay_y(i32(zz)).wait_send()
    for p in range(2, N):
        forward(i32(p)).wait_send()
    for p in range(1, N):
        result_copy(i32(p)).wait()
    result_own().wait()


def _tables():
    freq = float(THETA) ** (-np.arange(HEAD // 2, dtype=np.float64) / (HEAD // 2))
    freq = np.concatenate([freq, freq])
    loc = np.arange(BLK, dtype=np.float64)[:, None] * freq
    base = (np.arange(N, dtype=np.float64) * BLK)[:, None] * freq
    return (np.stack([np.cos(loc), np.sin(loc)]).astype(np.float32),
            np.concatenate([np.cos(base), np.sin(base)]).astype(np.float32))


def normed(x, gain):
    wide = x.astype(jnp.float32)
    scale = lax.rsqrt(jnp.mean(wide * wide, -1, keepdims=True) + 1e-6)
    return (wide * scale * gain.astype(jnp.float32)).astype(jnp.bfloat16)


def solution(mesh):
    loc, base = _tables()

    def step(x, gain, wq, wk, wv, wo):
        a = normed(x, gain)
        dma, any_ = pltpu.SemaphoreType.DMA, pl.BlockSpec(memory_space=pl.ANY)
        seen = pl.pallas_call(
            _mega,
            out_shape=jax.ShapeDtypeStruct((BLK, N * QW), jnp.bfloat16),
            in_specs=[any_] * 4 + [pl.BlockSpec(memory_space=pltpu.VMEM)] * 2,
            out_specs=any_,
            scratch_shapes=[
                pltpu.VMEM((N, BLK, DM), jnp.bfloat16),
                pltpu.VMEM((DM, QW + 2 * KW), jnp.bfloat16),
                pltpu.VMEM((N, 2, 2 * BLK, HEAD), jnp.bfloat16),
                pltpu.VMEM((N, 2, BLK, HEAD), jnp.bfloat16),
                pltpu.VMEM((N, 2, ROWS_V, BLK), jnp.bfloat16),
                pltpu.VMEM((N, 2, ROWS_V, 2 * BLK), jnp.float32),
                pltpu.VMEM((N, 2, 1, 2 * BLK), jnp.float32),
                pltpu.VMEM((N, BLK, QW), jnp.bfloat16),
                dma, dma((3,)), dma((N,)), dma((N,)), dma((2,)), dma((2,)),
                dma((2,)), dma((2, 2)), dma((2, 2)), dma((N,)), dma((N,)), dma((N,)), dma,
            ],
            compiler_params=pltpu.CompilerParams(collective_id=0, has_side_effects=True, vmem_limit_bytes=63 * 2**20),
            cost_estimate=pl.CostEstimate(flops=2 * 10**10 * 2, transcendentals=4 * 10**7, bytes_accessed=16 * 2**20),
        )(a, wq, wk, wv, jnp.asarray(loc), jnp.asarray(base))
        y = jnp.dot(seen, wo, preferred_element_type=jnp.float32)
        return (x.astype(jnp.float32) + y).astype(jnp.bfloat16)

    tokens, whole = P(("dp", "sp"), None), P(None, None)
    return jax.shard_map(step, mesh=mesh, in_specs=(tokens, P(None), whole, whole, whole, whole), out_specs=tokens, check_vma=False)
```

```python
import jax
import jax.numpy as jnp
import numpy as np
from jax import lax
from jax.experimental import pallas as pl
from jax.experimental.pallas import tpu as pltpu
from jax.sharding import PartitionSpec as P

MESH = pl.DeviceIdType.MESH
NEG = -1e30
HIDDEN = 2 * NEG
LOG2E = 1.4426950408889634
HEAD = 128
THETA = 10000
N = 8
BLK = 512
HALF = BLK // 2
QUARTER = BLK // 4
DM = 2048
QW = 512
KW = 256
ROWS_V = 144
SB = 2
KS, QS = 256, 512
TILE = 256


def _dot(a, b, ca, cb):
    return lax.dot_general(a, b, (((ca,), (cb,)), ((), ())), preferred_element_type=jnp.float32)


def _xor(a, b):
    bit = lambda v, w: lax.rem(lax.div(v, w), 2)
    return sum(lax.rem(bit(a, w) + bit(b, w), 2) * w for w in (4, 2, 1))


def _mega(x_hbm, gain_ref, wq_hbm, wk_hbm, wv_hbm, wo_hbm, loc_ref, base_ref, y_hbm,
          abuf, w, qt, k, vt, acc, top, res, sb, yacc,
          x_sem, w_sem, dsem, sibsem, qasem, qbsem, s_sib, s_dir, s_rel, s_fwd, s_o, osem, wo_sem, y_sem):
    i32 = lambda v: jnp.asarray(v, jnp.int32)
    d = lax.axis_index("sp").astype(jnp.int32)
    z = lax.rem(d, 2)
    nz = 1 - z
    sib, ynb, xnb = (_xor(d, i32(m)) for m in (1, 2, 4))
    e = HEAD**-0.5 * LOG2E

    def columns(ref, s, width):
        return ref.at[:, pl.ds(pl.multiple_of(s * width, width), width)]

    x_loads = [pltpu.make_async_copy(x_hbm.at[:, c * QW : (c + 1) * QW], res.at[N + c], x_sem.at[c]) for c in range(DM // QW)]
    w_loads = [
        pltpu.make_async_copy(columns(src, _xor(d, i32(6 * n)), width), w.at[n, :, at : at + width], w_sem.at[n, c])
        for n in range(2)
        for c, (src, at, width) in enumerate(((wq_hbm, 0, QW), (wk_hbm, QW, KW), (wv_hbm, QW + KW, KW)))
    ]
    for c in x_loads + w_loads:
        c.start()
    barrier = pltpu.get_barrier_semaphore()
    for m in range(1, N):
        pl.semaphore_signal(barrier, inc=1, device_id={"sp": _xor(d, i32(m))}, device_id_type=MESH)

    for c in x_loads:
        c.wait()
    gain = gain_ref[...].astype(jnp.float32)
    STEP = 64

    def norm(r, _):
        rows = pl.ds(pl.multiple_of(r * STEP, STEP), STEP)
        wide = jnp.concatenate([res[N + c, rows, :].astype(jnp.float32) for c in range(DM // QW)], axis=1)
        scale = lax.rsqrt(jnp.mean(wide * wide, -1, keepdims=True) + 1e-6)
        abuf[0, rows, :] = (wide * scale * gain).astype(jnp.bfloat16)
        return _

    lax.fori_loop(0, BLK // STEP, norm, None)
    pl.semaphore_wait(barrier, N - 1)

    def _xor1(zz):
        return lax.rem(zz + z, 2)

    def part(src, dst, at, rows, dev, ssem, rsem):
        here = pl.ds(pl.multiple_of(at, QUARTER), rows)
        return pltpu.make_async_remote_copy(abuf.at[src, here], abuf.at[dst, here], ssem, rsem, device_id={"sp": dev}, device_id_type=MESH)

    sib_a = part(0, 1, nz * HALF, HALF, sib, s_sib.at[0], dsem.at[1])
    sib_b = part(0, 1, z * HALF, HALF, sib, s_sib.at[1], sibsem.at[1])

    def to_y(zz):
        return part(_xor1(zz), 2 + _xor1(zz), z * HALF, HALF, ynb, s_dir.at[zz, 0], dsem.at[2 + _xor1(zz)])

    def to_x(zz):
        return part(_xor1(zz), 4 + _xor1(zz), z * HALF, HALF, xnb, s_dir.at[zz, 1], dsem.at[4 + _xor1(zz)])

    def relay_x(zz):
        return part(2 + _xor1(zz), 6 + _xor1(zz), z * HALF, QUARTER, xnb, s_rel.at[zz, 0], qasem.at[_xor1(zz)])

    def relay_y(zz):
        return part(4 + _xor1(zz), 6 + _xor1(zz), z * HALF + QUARTER, QUARTER, ynb, s_rel.at[zz, 1], qbsem.at[_xor1(zz)])

    def forward(p):
        return part(p, _xor(p, i32(1)), z * HALF, HALF, sib, s_fwd.at[p], sibsem.at[_xor(p, i32(1))])

    sib_a.start()

    @pl.when(z == 0)
    def _():
        to_y(i32(0)).start()
        to_x(i32(0)).start()

    sib_b.start()
    sib_a.wait_recv()

    @pl.when(z == 1)
    def _():
        to_y(i32(0)).start()
        to_x(i32(0)).start()

    to_y(i32(1)).start()
    to_x(i32(1)).start()
    for c in w_loads:
        c.wait()

    ones = jnp.ones((ROWS_V - HEAD, BLK), jnp.bfloat16)
    lane = lax.broadcasted_iota(jnp.int32, (BLK, HEAD), 1)

    def project(n, p, qi, with_q):
        s = _xor(d, p)
        cb, sb_ = base_ref[pl.ds(s, 1), :], base_ref[pl.ds(N + s, 1), :]
        cl, sl = loc_ref[0], loc_ref[1]
        cos = cb * cl - sb_ * sl
        sin = sb_ * cl + cb * sl
        sin = jnp.where(lane < HEAD // 2, -sin, sin)

        def turn(t):
            t = t.astype(jnp.bfloat16).astype(jnp.float32)
            return t * cos + pltpu.roll(t, HEAD // 2, 1) * sin

        def piece(c):
            y = _dot(abuf[p], w[n, :, c * 256 : (c + 1) * 256], 1, 0)
            return y[:, :HEAD], y[:, HEAD:]

        @pl.when(with_q)
        def _():
            for c in range(2):
                for m, t in enumerate(piece(c)):
                    qt[qi, c, :, m * BLK : (m + 1) * BLK] = turn(t).T.astype(jnp.bfloat16)
            top[qi] = jnp.full((2, 1, 2 * BLK), NEG, jnp.float32)
            acc[qi] = jnp.zeros((2, ROWS_V, 2 * BLK), jnp.float32)

        for m, t in enumerate(piece(2)):
            k[n, p, m] = turn(t).astype(jnp.bfloat16)
        for m, t in enumerate(piece(3)):
            vt[n, p, m, :HEAD, :] = t.T.astype(jnp.bfloat16)
            vt[n, p, m, HEAD:, :] = ones

    def attend(n, qi, pj, masked):
        if masked:
            ok = lax.broadcasted_iota(jnp.int32, (BLK, BLK), 1) >= lax.broadcasted_iota(jnp.int32, (BLK, BLK), 0)

        def scores(x):
            h, at = x // 2, x % 2 * BLK
            s = _dot(k[n, pj, h], qt[qi, h, :, at : at + BLK], 1, 0)
            if masked:
                s = jnp.where(ok, s, HIDDEN)
            sb[x % SB] = s
            old = top[qi, h, :, at : at + BLK]
            new = jnp.maximum(old, s.max(axis=0, keepdims=True))
            top[qi, h, :, at : at + BLK] = new
            return new, jnp.exp2((old - new) * e)

        def values(x, new, keep):
            h, at = x // 2, x % 2 * BLK
            for c0 in range(0, BLK, QS):
                cols = slice(c0, c0 + QS)
                part = None
                for k0 in range(0, BLK, KS):
                    keys = slice(k0, k0 + KS)
                    p = jnp.exp2((sb[x % SB, keys, cols] - new[:, cols]) * e).astype(jnp.bfloat16)
                    more = _dot(vt[n, pj, h, :, keys], p, 1, 0)
                    part = more if part is None else part + more
                here = slice(at + c0, at + c0 + QS)
                acc[qi, h, :, here] = acc[qi, h, :, here] * keep[:, cols] + part

        ready = [scores(0)]
        for x in range(4):
            if x < 3:
                ready.append(scores(x + 1))
            values(x, *ready[x])

    def group_of(p):
        r = lax.div(p, 2)
        return jnp.where(r == 0, 0, jnp.where(r == 3, 3, 1 + _xor1(lax.rem(p, 2))))

    def slot_of(g, u):
        return jnp.where(g == 0, u, jnp.where(g == 3, 6 + _xor1(u), 2 + 2 * u + _xor1(jnp.maximum(g - 1, 0))))

    def last_group(i):
        out = i32(0)
        for j in range(N):
            out = jnp.maximum(out, jnp.where(i32(j) <= i, group_of(_xor(d, i32(j))), 0))
        return out

    def result_copy(src, dst, dev, at):
        return pltpu.make_async_remote_copy(res.at[src], res.at[dst], s_o.at[at], osem.at[dst], device_id={"sp": dev}, device_id_type=MESH)

    def finish(qi, g):
        second = qi >= 6
        slot = jnp.where(second, qi - 6, qi)

        @pl.when(last_group(_xor(d, slot)) == g)
        def _():
            to = jnp.where(slot == 0, qi, jnp.where(second, N, N + slot))
            for h in range(2):
                for n in range(2):
                    cols = slice(n * BLK, (n + 1) * BLK)
                    total = acc[qi, h, HEAD : HEAD + 1, cols]
                    o = (acc[qi, h, :HEAD, cols] * (1 / total)).T
                    res[to, :, (2 * h + n) * HEAD : (2 * h + n + 1) * HEAD] = o.astype(jnp.bfloat16)

            @pl.when(slot != 0)
            def _():
                result_copy(to, qi, _xor(d, slot), to - N).start()

    def wo_load(p):
        rows = pl.ds(pl.multiple_of(_xor(d, i32(p)) * QW, QW), QW)
        return pltpu.make_async_copy(wo_hbm.at[rows, :], abuf.at[p], wo_sem.at[p])

    def x_load(h):
        return pltpu.make_async_copy(x_hbm.at[:, h * 1024 : (h + 1) * 1024], w.at[0, h * BLK : (h + 1) * BLK, :], x_sem.at[h])

    def group(g, _):
        @pl.when((g == 1) | (g == 2))
        def _():
            zz = g - 1
            ps, px = 2 + _xor1(zz), 4 + _xor1(zz)
            to_y(zz).wait_recv()
            relay_x(zz).start()
            forward(ps).start()
            to_x(zz).wait_recv()
            relay_y(zz).start()
            forward(px).start()

        def chip(p):
            return lax.div(_xor(d, p), 2)

        def arrive(x, _):
            n, u = lax.div(x, 2), lax.rem(x, 2)
            p = slot_of(g, u)

            @pl.when((g == 3) & (n == 0))
            def _():
                relay_x(u).wait_recv()
                relay_y(u).wait_recv()
                forward(p).start()

            @pl.when((p != 0) & (n == 0))
            def _():
                part(0, p, nz * HALF, HALF, sib, s_sib.at[0], sibsem.at[p]).wait_recv()

            @pl.when((n == 0) | (chip(p) <= lax.div(d, 2)))
            def _():
                project(n, p, jnp.where(n == 0, jnp.minimum(p, 5), 6 + jnp.minimum(p, 1)), jnp.where(n == 0, g < 3, g == 0))

            return _

        lax.fori_loop(0, 4, arrive, None)
        p0, p1 = slot_of(g, i32(0)), slot_of(g, i32(1))

        @pl.when(g == 3)
        def _():
            sib_a.wait_send()
            sib_b.wait_send()
            for zz in range(2):
                to_y(i32(zz)).wait_send()
                to_x(i32(zz)).wait_send()
                relay_x(i32(zz)).wait_send()
                relay_y(i32(zz)).wait_send()
            for p in range(2, N):
                forward(i32(p)).wait_send()
            for p in (0, 6, 1, 7, 2, 4, 3, 5):
                wo_load(p).start()
            for h in range(2):
                x_load(h).start()

        b0, b1 = _xor(d, p0), _xor(d, p1)
        hi, lo = jnp.where(b0 > b1, p0, p1), jnp.where(b0 > b1, p1, p0)
        old = 4 * g

        def pair(x, _):
            t, u = jnp.maximum(2 * g - 1 - lax.div(x, 2), 0), lax.rem(x, 2)
            told = slot_of(lax.div(t, 2), lax.rem(t, 2))
            new = jnp.where(u == 0, p0, p1)
            up = _xor(d, told) > _xor(d, new)
            y = jnp.maximum(x - old - 1, 0)
            y0, y1 = lax.div(y, 2), lax.rem(y, 2)
            newy = jnp.where(y1 == 0, p0, p1)
            is_old, is_in = x < old, x == old
            first = g == 0
            qi = jnp.where(is_old, jnp.where(up, told, new), jnp.where(is_in, hi, jnp.where(first, 6 + hi, 6 + y0)))
            pj = jnp.where(is_old, jnp.where(up, new, told), jnp.where(is_in | first, lo, newy))
            seen = jnp.where(first, (y == 0).astype(jnp.int32), (chip(newy) < lax.div(d, 2)).astype(jnp.int32))
            early = (g < 3).astype(jnp.int32)
            active = jnp.where(is_old, jnp.maximum(up.astype(jnp.int32), early), jnp.where(is_in, early, seen))

            @pl.when(active == 1)
            def _():
                attend(jnp.where(x > old, 1, 0), qi, pj, False)

            done = jnp.where(is_old, u == 1, (x > old) & (y1 == 1) & (g > 0))

            @pl.when(done)
            def _():
                finish(jnp.where(is_old, told, 6 + y0), g)

            return _

        lax.fori_loop(0, old + jnp.where(g == 0, 2, 5), pair, None)

        def diagonal(x, _):
            n, u = lax.div(x, 2), lax.rem(x, 2)
            p = jnp.where(u == 0, p0, p1)
            qi = jnp.where(n == 0, p, 6 + u)
            attend(n, qi, p, True)
            finish(qi, g)
            return _

        lax.fori_loop(0, jnp.where(g == 0, 4, jnp.where(g == 3, 0, 2)), diagonal, None)
        return _

    lax.fori_loop(0, 4, group, None)

    def output(sets, start, end):
        for p in sets:
            wo_load(p).wait()
            if p not in (0, 6):
                result_copy(0, p, sib, 0).wait_recv()

        def tile(t, _):
            cols = pl.ds(pl.multiple_of(t * TILE, TILE), TILE)
            y = None
            for p in sets:
                more = _dot(res[p], abuf[p, :, cols], 1, 0)
                y = more if y is None else y + more
            if not start:
                y = y + yacc[:, cols]
            if not end:
                yacc[:, cols] = y
            else:
                half, at = lax.div(t, 4), pl.ds(pl.multiple_of(lax.rem(t, 4) * TILE, TILE), TILE)
                rows = pl.ds(pl.multiple_of(half * BLK, BLK), BLK)
                w[1, rows, at] = (w[0, rows, at].astype(jnp.float32) + y).astype(jnp.bfloat16)
                y_store(t).start()
            return _

        lax.fori_loop(0, DM // TILE, tile, None)

    def y_store(t):
        half, at = lax.div(t, 4), pl.ds(pl.multiple_of(lax.rem(t, 4) * TILE, TILE), TILE)
        rows = pl.ds(pl.multiple_of(half * BLK, BLK), BLK)
        return pltpu.make_async_copy(w.at[1, rows, at], columns(y_hbm, t, TILE), y_sem.at[t])

    output((0, 6, 1, 7), True, False)
    for h in range(2):
        x_load(h).wait()
    output((2, 4), False, False)
    output((3, 5), False, True)
    for t in range(DM // TILE):
        y_store(i32(t)).wait()
    for at in range(6):
        result_copy(0, 1, sib, at).wait_send()


def _tables():
    freq = float(THETA) ** (-np.arange(HEAD // 2, dtype=np.float64) / (HEAD // 2))
    freq = np.concatenate([freq, freq])
    loc = np.arange(BLK, dtype=np.float64)[:, None] * freq
    base = (np.arange(N, dtype=np.float64) * BLK)[:, None] * freq
    return (np.stack([np.cos(loc), np.sin(loc)]).astype(np.float32),
            np.concatenate([np.cos(base), np.sin(base)]).astype(np.float32))


def solution(mesh):
    loc, base = _tables()

    def step(x, gain, wq, wk, wv, wo):
        dma, any_, vmem = pltpu.SemaphoreType.DMA, pl.BlockSpec(memory_space=pl.ANY), pl.BlockSpec(memory_space=pltpu.VMEM)
        return pl.pallas_call(
            _mega,
            out_shape=jax.ShapeDtypeStruct((BLK, DM), jnp.bfloat16),
            in_specs=[any_, vmem, any_, any_, any_, any_, vmem, vmem],
            out_specs=any_,
            scratch_shapes=[
                pltpu.VMEM((N, BLK, DM), jnp.bfloat16),
                pltpu.VMEM((2, DM, QW + 2 * KW), jnp.bfloat16),
                pltpu.VMEM((N, 2, HEAD, 2 * BLK), jnp.bfloat16),
                pltpu.VMEM((2, N, 2, BLK, HEAD), jnp.bfloat16),
                pltpu.VMEM((2, N, 2, ROWS_V, BLK), jnp.bfloat16),
                pltpu.VMEM((N, 2, ROWS_V, 2 * BLK), jnp.float32),
                pltpu.VMEM((N, 2, 1, 2 * BLK), jnp.float32),
                pltpu.VMEM((N + 6, BLK, QW), jnp.bfloat16),
                pltpu.VMEM((SB, BLK, BLK), jnp.float32),
                pltpu.VMEM((BLK, DM), jnp.float32),
                dma((4,)), dma((2, 3)), dma((N,)), dma((N,)), dma((2,)), dma((2,)),
                dma((2,)), dma((2, 2)), dma((2, 2)), dma((N,)), dma((6,)), dma((N,)), dma((N,)), dma((N,)),
            ],
            compiler_params=pltpu.CompilerParams(collective_id=0, has_side_effects=True, vmem_limit_bytes=67043328),
            cost_estimate=pl.CostEstimate(flops=6 * 10**10, transcendentals=4 * 10**7, bytes_accessed=64 * 2**20),
        )(x, gain.reshape(1, DM), wq, wk, wv, wo, jnp.asarray(loc), jnp.asarray(base))

    tokens, whole = P(("dp", "sp"), None), P(None, None)
    return jax.shard_map(step, mesh=mesh, in_specs=(tokens, P(None), whole, whole, whole, whole), out_specs=tokens, check_vma=False)
```

```python
import jax
import jax.numpy as jnp
import numpy as np
from jax import lax
from jax.experimental import pallas as pl
from jax.experimental.pallas import tpu as pltpu
from jax.sharding import PartitionSpec as P

MESH = pl.DeviceIdType.MESH
NEG = -1e30
HIDDEN = 2 * NEG
LOG2E = 1.4426950408889634
HEAD = 128
THETA = 10000
N = 8
BLK = 512
HALF = BLK // 2
QUARTER = BLK // 4
DM = 2048
QW = 512
KW = 256
ROWS_V = 144
AHEAD = 2
SB = AHEAD + 1
KS = 256
TILE = 256


def _dot(a, b, ca, cb):
    return lax.dot_general(a, b, (((ca,), (cb,)), ((), ())), preferred_element_type=jnp.float32)


def _xor(a, b):
    bit = lambda v, w: lax.rem(lax.div(v, w), 2)
    return sum(lax.rem(bit(a, w) + bit(b, w), 2) * w for w in (4, 2, 1))


def _mega(x_hbm, gain_ref, wq_hbm, wk_hbm, wv_hbm, wo_hbm, loc_ref, base_ref, y_hbm,
          abuf, w, qt, k, vt, acc, top, res, sb, yacc,
          x_sem, w_sem, dsem, sibsem, qasem, qbsem, s_sib, s_dir, s_rel, s_fwd, s_o, osem, wo_sem, y_sem):
    i32 = lambda v: jnp.asarray(v, jnp.int32)
    d = lax.axis_index("sp").astype(jnp.int32)
    z = lax.rem(d, 2)
    nz = 1 - z
    sib, ynb, xnb = (_xor(d, i32(m)) for m in (1, 2, 4))
    e = HEAD**-0.5 * LOG2E

    def columns(ref, s, width):
        return ref.at[:, pl.ds(pl.multiple_of(s * width, width), width)]

    x_loads = [pltpu.make_async_copy(x_hbm.at[:, c * QW : (c + 1) * QW], res.at[N + c], x_sem.at[c]) for c in range(DM // QW)]
    w_loads = [
        pltpu.make_async_copy(columns(src, _xor(d, i32(6 * n)), width), w.at[n, :, at : at + width], w_sem.at[n, c])
        for n in range(2)
        for c, (src, at, width) in enumerate(((wq_hbm, 0, QW), (wk_hbm, QW, KW), (wv_hbm, QW + KW, KW)))
    ]
    for c in x_loads + w_loads[:3]:
        c.start()
    barrier = pltpu.get_barrier_semaphore()
    for m in range(1, N):
        pl.semaphore_signal(barrier, inc=1, device_id={"sp": _xor(d, i32(m))}, device_id_type=MESH)

    for c in x_loads:
        c.wait()
    gain = gain_ref[...].astype(jnp.float32).reshape(1, DM)
    STEP = 64

    def norm(r, _):
        rows = pl.ds(pl.multiple_of(r * STEP, STEP), STEP)
        wide = jnp.concatenate([res[N + c, rows, :].astype(jnp.float32) for c in range(DM // QW)], axis=1)
        scale = lax.rsqrt(jnp.mean(wide * wide, -1, keepdims=True) + 1e-6)
        abuf[0, rows, :] = (wide * scale * gain).astype(jnp.bfloat16)
        return _

    lax.fori_loop(0, BLK // STEP, norm, None)
    pl.semaphore_wait(barrier, N - 1)

    def _xor1(zz):
        return lax.rem(zz + z, 2)

    def part(src, dst, at, rows, dev, ssem, rsem):
        here = pl.ds(pl.multiple_of(at, QUARTER), rows)
        return pltpu.make_async_remote_copy(abuf.at[src, here], abuf.at[dst, here], ssem, rsem, device_id={"sp": dev}, device_id_type=MESH)

    sib_a = part(0, 1, nz * HALF, HALF, sib, s_sib.at[0], dsem.at[1])
    sib_b = part(0, 1, z * HALF, HALF, sib, s_sib.at[1], sibsem.at[1])

    def to_y(zz):
        return part(_xor1(zz), 2 + _xor1(zz), z * HALF, HALF, ynb, s_dir.at[zz, 0], dsem.at[2 + _xor1(zz)])

    def to_x(zz):
        return part(_xor1(zz), 4 + _xor1(zz), z * HALF, HALF, xnb, s_dir.at[zz, 1], dsem.at[4 + _xor1(zz)])

    def relay_x(zz):
        return part(2 + _xor1(zz), 6 + _xor1(zz), z * HALF, QUARTER, xnb, s_rel.at[zz, 0], qasem.at[_xor1(zz)])

    def relay_y(zz):
        return part(4 + _xor1(zz), 6 + _xor1(zz), z * HALF + QUARTER, QUARTER, ynb, s_rel.at[zz, 1], qbsem.at[_xor1(zz)])

    def forward(p):
        return part(p, _xor(p, i32(1)), z * HALF, HALF, sib, s_fwd.at[p], sibsem.at[_xor(p, i32(1))])

    sib_a.start()

    @pl.when(z == 0)
    def _():
        to_y(i32(0)).start()
        to_x(i32(0)).start()

    sib_b.start()
    sib_a.wait_recv()

    @pl.when(z == 1)
    def _():
        to_y(i32(0)).start()
        to_x(i32(0)).start()

    to_y(i32(1)).start()
    to_x(i32(1)).start()
    for c in w_loads[3:]:
        c.start()
    ones = jnp.ones((ROWS_V - HEAD, BLK), jnp.bfloat16)
    lane = lax.broadcasted_iota(jnp.int32, (BLK, HEAD), 1)

    def project(n, p, qi, with_q):
        s = _xor(d, p)
        cb, sb_ = base_ref[pl.ds(s, 1), :], base_ref[pl.ds(N + s, 1), :]
        cl, sl = loc_ref[0], loc_ref[1]
        cos = cb * cl - sb_ * sl
        sin = sb_ * cl + cb * sl
        sin = jnp.where(lane < HEAD // 2, -sin, sin)

        def turn(t):
            t = t.astype(jnp.bfloat16).astype(jnp.float32)
            return t * cos + pltpu.roll(t, HEAD // 2, 1) * sin

        def piece(c):
            y = _dot(abuf[p], w[n, :, c * 256 : (c + 1) * 256], 1, 0)
            return y[:, :HEAD], y[:, HEAD:]

        @pl.when(with_q)
        def _():
            for c in range(2):
                for m, t in enumerate(piece(c)):
                    qt[qi, c, :, m * BLK : (m + 1) * BLK] = turn(t).T.astype(jnp.bfloat16)
            top[qi] = jnp.full((2, 1, 2 * BLK), NEG, jnp.float32)
            acc[qi] = jnp.zeros((2, ROWS_V, 2 * BLK), jnp.float32)

        for m, t in enumerate(piece(2)):
            k[n, p, m] = turn(t).astype(jnp.bfloat16)
        for m, t in enumerate(piece(3)):
            vt[n, p, m, :HEAD, :] = t.T.astype(jnp.bfloat16)
            vt[n, p, m, HEAD:, :] = ones

    def attend(items, masked):
        pieces = []
        for it in items:
            for h in range(2):
                for m in range(2):
                    if masked:
                        pieces += [(it, h, m * BLK, HALF, HALF), (it, h, m * BLK + HALF, HALF, BLK)]
                    else:
                        pieces += [(it, h, m * BLK, BLK, BLK)]

        def scores(x):
            (n, qi, pj), h, at, wide, keys = pieces[x]
            cols = slice(at, at + wide)
            s = _dot(k[n, pj, h, :keys, :], qt[qi, h, :, cols], 1, 0)
            if masked:
                iota = lambda axis: lax.broadcasted_iota(jnp.int32, (keys, wide), axis)
                s = jnp.where(iota(1) + (at % BLK) >= iota(0), s, HIDDEN)
            sb[x % SB, :keys, :wide] = s
            old = top[qi, h, :, cols]
            new = jnp.maximum(old, s.max(axis=0, keepdims=True))
            top[qi, h, :, cols] = new
            return new, jnp.exp2((old - new) * e)

        def values(x, new, keep):
            (n, qi, pj), h, at, wide, keys = pieces[x]
            cols = slice(at, at + wide)
            part = None
            for k0 in range(0, keys, KS):
                p = jnp.exp2((sb[x % SB, k0 : k0 + KS, :wide] - new) * e).astype(jnp.bfloat16)
                more = _dot(vt[n, pj, h, :, k0 : k0 + KS], p, 1, 0)
                part = more if part is None else part + more
            acc[qi, h, :, cols] = acc[qi, h, :, cols] * keep + part

        ready = [scores(x) for x in range(AHEAD)]
        for x in range(len(pieces)):
            if x + AHEAD < len(pieces):
                ready.append(scores(x + AHEAD))
            values(x, *ready[x])

    def group_of(p):
        r = lax.div(p, 2)
        return jnp.where(r == 0, 0, jnp.where(r == 3, 3, 1 + _xor1(lax.rem(p, 2))))

    def slot_of(g, u):
        return jnp.where(g == 0, u, jnp.where(g == 3, 6 + _xor1(u), 2 + 2 * u + _xor1(jnp.maximum(g - 1, 0))))

    def last_group(i):
        out = i32(0)
        for j in range(N):
            out = jnp.maximum(out, jnp.where(i32(j) <= i, group_of(_xor(d, i32(j))), 0))
        return out

    def result_copy(src, dst, dev, at):
        return pltpu.make_async_remote_copy(res.at[src], res.at[dst], s_o.at[at], osem.at[dst], device_id={"sp": dev}, device_id_type=MESH)

    def finish(qi, g):
        second = qi >= 6
        slot = jnp.where(second, qi - 6, qi)

        last = last_group(_xor(d, slot))

        @pl.when(jnp.where(second & (last == 3), 4, last) == g)
        def _():
            to = jnp.where(slot == 0, qi, jnp.where(second, N, N + slot))
            for h in range(2):
                for n in range(2):
                    cols = slice(n * BLK, (n + 1) * BLK)
                    total = acc[qi, h, HEAD : HEAD + 1, cols]
                    o = (acc[qi, h, :HEAD, cols] * (1 / total)).T
                    res[to, :, (2 * h + n) * HEAD : (2 * h + n + 1) * HEAD] = o.astype(jnp.bfloat16)

            @pl.when(slot != 0)
            def _():
                result_copy(to, qi, _xor(d, slot), to - N).start()

    def wo_load(p):
        rows = pl.ds(pl.multiple_of(_xor(d, jnp.asarray(p, jnp.int32)) * QW, QW), QW)
        return pltpu.make_async_copy(wo_hbm.at[rows, :], abuf.at[p], wo_sem.at[p])

    def x_load(h):
        return pltpu.make_async_copy(x_hbm.at[:, h * 1024 : (h + 1) * 1024], w.at[0, h * BLK : (h + 1) * BLK, :], x_sem.at[h])

    def group(g, _):
        @pl.when((g == 1) | (g == 2))
        def _():
            zz = g - 1
            ps, px = 2 + _xor1(zz), 4 + _xor1(zz)
            to_y(zz).wait_recv()
            relay_x(zz).start()
            forward(ps).start()
            to_x(zz).wait_recv()
            relay_y(zz).start()
            forward(px).start()

        def chip(p):
            return lax.div(_xor(d, p), 2)

        tail = g == 4

        def arrive(x, _):
            half, u = lax.div(x, 2), lax.rem(x, 2)
            n = jnp.where(tail, 1, half)
            p = slot_of(jnp.where(tail, 3, g), u)

            for m in range(2):

                @pl.when((g == 0) & (x == 2 * m))
                def _():
                    for c in w_loads[3 * m : 3 * m + 3]:
                        c.wait()

            @pl.when((g == 3) & (n == 0))
            def _():
                relay_x(u).wait_recv()
                relay_y(u).wait_recv()
                forward(p).start()

            @pl.when((p != 0) & (n == 0))
            def _():
                part(0, p, nz * HALF, HALF, sib, s_sib.at[0], sibsem.at[p]).wait_recv()

            @pl.when(jnp.where(n == 0, (g < 3) | (d >= 2), ((g < 3) | (tail & (half == 0))) & (chip(p) <= lax.div(d, 2))))
            def _():
                project(n, p, jnp.where(n == 0, jnp.minimum(p, 5), 6 + jnp.minimum(p, 1)), jnp.where(n == 0, g < 3, g == 0))

            return _

        lax.fori_loop(0, 4, arrive, None)
        p0, p1 = slot_of(g, i32(0)), slot_of(g, i32(1))

        @pl.when(g == 3)
        def _():
            sib_a.wait_send()
            sib_b.wait_send()
            for zz in range(2):
                to_y(i32(zz)).wait_send()
                to_x(i32(zz)).wait_send()
                relay_x(i32(zz)).wait_send()
                relay_y(i32(zz)).wait_send()
            for p in range(2, 6):
                forward(i32(p)).wait_send()
            for p in range(6):
                wo_load(p).start()
            for h in range(2):
                x_load(h).start()

        @pl.when(tail)
        def _():
            for p in (6, 7):
                forward(i32(p)).wait_send()
                wo_load(p).start()

        b0, b1 = _xor(d, p0), _xor(d, p1)
        hi, lo = jnp.where(b0 > b1, p0, p1), jnp.where(b0 > b1, p1, p0)
        first = g == 0
        old = jnp.where(tail, 0, 2 * g)

        def pair(x, _):
            t = jnp.maximum(old - 1 - x, 0)
            told = slot_of(lax.div(t, 2), lax.rem(t, 2))
            is_old = x < old
            newy = jnp.where(tail, slot_of(3, x), jnp.where(x == old, p0, p1))
            ups = [_xor(d, told) > _xor(d, p) for p in (p0, p1)]
            qs = [jnp.where(first, o, jnp.where(is_old, jnp.where(up, told, p), m)) for o, up, p, m in zip((hi, 6 + hi), ups, (p0, p1), (6, 7))]
            ks = [jnp.where(first, lo, jnp.where(is_old, jnp.where(up, p, told), newy)) for up, p in zip(ups, (p0, p1))]
            sets = [jnp.where(first, o, jnp.where(is_old, 0, 1)) for o in (0, 1)]
            seen = (chip(newy) < lax.div(d, 2)).astype(jnp.int32)
            wanted = jnp.where(is_old, jnp.maximum(ups[0].astype(jnp.int32), (g < 3).astype(jnp.int32)), jnp.maximum(seen, first.astype(jnp.int32)))

            @pl.when(wanted == 1)
            def _():
                attend([(sets[0], qs[0], ks[0]), (sets[1], qs[1], ks[1])], False)

            @pl.when(is_old)
            def _():
                finish(told, g)

            return _

        lax.fori_loop(0, old + jnp.where(first, 1, jnp.where(g == 3, 0, 2)), pair, None)

        @pl.when((g == 1) | (g == 2))
        def _():
            attend([(0, hi, lo)], False)

        def diagonal(n, _):
            attend([(n, jnp.where(n == 0, p, 6 + u), p) for u, p in enumerate((p0, p1))], True)
            return _

        lax.fori_loop(0, jnp.where(first, 2, jnp.where(g >= 3, 0, 1)), diagonal, None)

        def close(x, _):
            qi = jnp.where(x < 2, jnp.where(x == 0, p0, p1), 4 + x)

            @pl.when((x >= 2) | (g < 3))
            def _():
                finish(qi, g)

            return _

        lax.fori_loop(0, 4, close, None)
        return _

    lax.fori_loop(0, 5, group, None)

    def output(sets, start, end):
        for p in sets:
            wo_load(p).wait()
            if not (isinstance(p, int) and p in (0, 6)):
                result_copy(0, p, sib, 0).wait_recv()

        def tile(t, _):
            cols = pl.ds(pl.multiple_of(t * TILE, TILE), TILE)
            y = None
            for p in sets:
                more = _dot(res[p], abuf[p, :, cols], 1, 0)
                y = more if y is None else y + more
            if not start:
                y = y + yacc[:, cols]
            if not end:
                yacc[:, cols] = y
            else:
                half, at = lax.div(t, 4), pl.ds(pl.multiple_of(lax.rem(t, 4) * TILE, TILE), TILE)
                rows = pl.ds(pl.multiple_of(half * BLK, BLK), BLK)
                w[1, rows, at] = (w[0, rows, at].astype(jnp.float32) + y).astype(jnp.bfloat16)
                y_store(t).start()
            return _

        lax.fori_loop(0, DM // TILE, tile, None)

    def y_store(t):
        half, at = lax.div(t, 4), pl.ds(pl.multiple_of(lax.rem(t, 4) * TILE, TILE), TILE)
        rows = pl.ds(pl.multiple_of(half * BLK, BLK), BLK)
        return pltpu.make_async_copy(w.at[1, rows, at], columns(y_hbm, t, TILE), y_sem.at[t])

    output((0, 6, 1, 7), True, False)
    for h in range(2):
        x_load(h).wait()
    near = jnp.where(lax.div(d, 2) == 2, 4, 2)
    output((near, near + 1), False, False)
    output((6 - near, 7 - near), False, True)
    for t in range(DM // TILE):
        y_store(i32(t)).wait()
    for at in range(6):
        result_copy(0, 1, sib, at).wait_send()


def _tables():
    freq = float(THETA) ** (-np.arange(HEAD // 2, dtype=np.float64) / (HEAD // 2))
    freq = np.concatenate([freq, freq])
    loc = np.arange(BLK, dtype=np.float64)[:, None] * freq
    base = (np.arange(N, dtype=np.float64) * BLK)[:, None] * freq
    return (np.stack([np.cos(loc), np.sin(loc)]).astype(np.float32),
            np.concatenate([np.cos(base), np.sin(base)]).astype(np.float32))


def solution(mesh):
    loc, base = _tables()

    def step(x, gain, wq, wk, wv, wo):
        dma, any_, vmem = pltpu.SemaphoreType.DMA, pl.BlockSpec(memory_space=pl.ANY), pl.BlockSpec(memory_space=pltpu.VMEM)
        return pl.pallas_call(
            _mega,
            out_shape=jax.ShapeDtypeStruct((BLK, DM), jnp.bfloat16),
            in_specs=[any_, vmem, any_, any_, any_, any_, vmem, vmem],
            out_specs=any_,
            scratch_shapes=[
                pltpu.VMEM((N, BLK, DM), jnp.bfloat16),
                pltpu.VMEM((2, DM, QW + 2 * KW), jnp.bfloat16),
                pltpu.VMEM((N, 2, HEAD, 2 * BLK), jnp.bfloat16),
                pltpu.VMEM((2, N, 2, BLK, HEAD), jnp.bfloat16),
                pltpu.VMEM((2, N, 2, ROWS_V, BLK), jnp.bfloat16),
                pltpu.VMEM((N, 2, ROWS_V, 2 * BLK), jnp.float32),
                pltpu.VMEM((N, 2, 1, 2 * BLK), jnp.float32),
                pltpu.VMEM((N + 6, BLK, QW), jnp.bfloat16),
                pltpu.VMEM((SB, BLK, BLK), jnp.float32),
                pltpu.VMEM((BLK, DM), jnp.float32),
                dma((4,)), dma((2, 3)), dma((N,)), dma((N,)), dma((2,)), dma((2,)),
                dma((2,)), dma((2, 2)), dma((2, 2)), dma((N,)), dma((6,)), dma((N,)), dma((N,)), dma((N,)),
            ],
            compiler_params=pltpu.CompilerParams(collective_id=0, has_side_effects=True, vmem_limit_bytes=67043328),
            cost_estimate=pl.CostEstimate(flops=6 * 10**10, transcendentals=4 * 10**7, bytes_accessed=64 * 2**20),
        )(x, gain, wq, wk, wv, wo, jnp.asarray(loc), jnp.asarray(base))

    tokens, whole = P(("dp", "sp"), None), P(None, None)
    return jax.shard_map(step, mesh=mesh, in_specs=(tokens, P(None), whole, whole, whole, whole), out_specs=tokens, check_vma=False)
```

```python
import jax
import jax.numpy as jnp
import numpy as np
from jax import lax
from jax.experimental import pallas as pl
from jax.experimental.pallas import tpu as pltpu
from jax.sharding import PartitionSpec as P

MESH = pl.DeviceIdType.MESH
NEG = -1e30
HIDDEN = 2 * NEG
LOG2E = 1.4426950408889634
HEAD = 128
THETA = 10000
N = 8
BLK = 512
HALF = BLK // 2
QUARTER = BLK // 4
DM = 2048
QW = 512
KW = 256
ROWS_V = 144
AHEAD = 2
SB = AHEAD + 1
KS = 256
TILE = 256


def _dot(a, b, ca, cb):
    return lax.dot_general(a, b, (((ca,), (cb,)), ((), ())), preferred_element_type=jnp.float32)


def _xor(a, b):
    bit = lambda v, w: lax.rem(lax.div(v, w), 2)
    return sum(lax.rem(bit(a, w) + bit(b, w), 2) * w for w in (4, 2, 1))


def _mega(x_hbm, gain_ref, wq_hbm, wk_hbm, wv_hbm, wo_hbm, loc_ref, base_ref, y_hbm,
          abuf, w, qt, k, vt, acc, top, res, sb, yacc,
          x_sem, w_sem, dsem, sibsem, qasem, qbsem, s_sib, s_dir, s_rel, s_fwd, s_o, osem, wo_sem, y_sem):
    i32 = lambda v: jnp.asarray(v, jnp.int32)
    d = lax.axis_index("sp").astype(jnp.int32)
    z = lax.rem(d, 2)
    nz = 1 - z
    sib, ynb, xnb = (_xor(d, i32(m)) for m in (1, 2, 4))
    e = HEAD**-0.5 * LOG2E

    def columns(ref, s, width):
        return ref.at[:, pl.ds(pl.multiple_of(s * width, width), width)]

    x_loads = [pltpu.make_async_copy(x_hbm.at[:, c * QW : (c + 1) * QW], res.at[N + c], x_sem.at[c]) for c in range(DM // QW)]
    w_loads = [
        pltpu.make_async_copy(columns(src, _xor(d, i32(6 * n)), width), w.at[n, :, at : at + width], w_sem.at[n, c])
        for n in range(2)
        for c, (src, at, width) in enumerate(((wq_hbm, 0, QW), (wk_hbm, QW, KW), (wv_hbm, QW + KW, KW)))
    ]
    for c in x_loads + w_loads[:3]:
        c.start()
    barrier = pltpu.get_barrier_semaphore()
    for m in range(1, N):
        pl.semaphore_signal(barrier, inc=1, device_id={"sp": _xor(d, i32(m))}, device_id_type=MESH)

    for c in x_loads:
        c.wait()
    gain = gain_ref[...].astype(jnp.float32).reshape(1, DM)
    STEP = 64

    def norm(r, _):
        rows = pl.ds(pl.multiple_of(r * STEP, STEP), STEP)
        wide = jnp.concatenate([res[N + c, rows, :].astype(jnp.float32) for c in range(DM // QW)], axis=1)
        scale = lax.rsqrt(jnp.mean(wide * wide, -1, keepdims=True) + 1e-6)
        abuf[0, rows, :] = (wide * scale * gain).astype(jnp.bfloat16)
        return _

    lax.fori_loop(0, BLK // STEP, norm, None)
    pl.semaphore_wait(barrier, N - 1)

    def _xor1(zz):
        return lax.rem(zz + z, 2)

    def part(src, dst, at, rows, dev, ssem, rsem):
        here = pl.ds(pl.multiple_of(at, QUARTER), rows)
        return pltpu.make_async_remote_copy(abuf.at[src, here], abuf.at[dst, here], ssem, rsem, device_id={"sp": dev}, device_id_type=MESH)

    sib_a = part(0, 1, nz * HALF, HALF, sib, s_sib.at[0], dsem.at[1])
    sib_b = part(0, 1, z * HALF, HALF, sib, s_sib.at[1], sibsem.at[1])

    def to_y(zz):
        return part(_xor1(zz), 2 + _xor1(zz), z * HALF, HALF, ynb, s_dir.at[zz, 0], dsem.at[2 + _xor1(zz)])

    def to_x(zz):
        return part(_xor1(zz), 4 + _xor1(zz), z * HALF, HALF, xnb, s_dir.at[zz, 1], dsem.at[4 + _xor1(zz)])

    def relay_x(zz):
        return part(2 + _xor1(zz), 6 + _xor1(zz), z * HALF, QUARTER, xnb, s_rel.at[zz, 0], qasem.at[_xor1(zz)])

    def relay_y(zz):
        return part(4 + _xor1(zz), 6 + _xor1(zz), z * HALF + QUARTER, QUARTER, ynb, s_rel.at[zz, 1], qbsem.at[_xor1(zz)])

    def forward(p):
        return part(p, _xor(p, i32(1)), z * HALF, HALF, sib, s_fwd.at[p], sibsem.at[_xor(p, i32(1))])

    sib_a.start()

    @pl.when(z == 0)
    def _():
        to_y(i32(0)).start()
        to_x(i32(0)).start()

    sib_b.start()
    sib_a.wait_recv()

    @pl.when(z == 1)
    def _():
        to_y(i32(0)).start()
        to_x(i32(0)).start()

    to_y(i32(1)).start()
    to_x(i32(1)).start()
    for c in w_loads[3:]:
        c.start()
    ones = jnp.ones((ROWS_V - HEAD, BLK), jnp.bfloat16)
    lane = lax.broadcasted_iota(jnp.int32, (BLK, HEAD), 1)

    def project(n, p, qi, with_q):
        s = _xor(d, p)
        cb, sb_ = base_ref[pl.ds(s, 1), :], base_ref[pl.ds(N + s, 1), :]
        cl, sl = loc_ref[0], loc_ref[1]
        cos = cb * cl - sb_ * sl
        sin = sb_ * cl + cb * sl
        sin = jnp.where(lane < HEAD // 2, -sin, sin)

        def turn(t):
            t = t.astype(jnp.bfloat16).astype(jnp.float32)
            return t * cos + pltpu.roll(t, HEAD // 2, 1) * sin

        def piece(c):
            y = _dot(abuf[p], w[n, :, c * 256 : (c + 1) * 256], 1, 0)
            return y[:, :HEAD], y[:, HEAD:]

        @pl.when(with_q)
        def _():
            for c in range(2):
                for m, t in enumerate(piece(c)):
                    qt[qi, c, :, m * BLK : (m + 1) * BLK] = turn(t).T.astype(jnp.bfloat16)
            top[qi] = jnp.full((2, 1, 2 * BLK), NEG, jnp.float32)
            acc[qi] = jnp.zeros((2, ROWS_V, 2 * BLK), jnp.float32)

        for m, t in enumerate(piece(2)):
            k[n, p, m] = turn(t).astype(jnp.bfloat16)
        for m, t in enumerate(piece(3)):
            vt[n, p, m, :HEAD, :] = t.T.astype(jnp.bfloat16)
            vt[n, p, m, HEAD:, :] = ones

    def attend(items, masked):
        pieces = []
        for it in items:
            for h in range(2):
                for m in range(2):
                    if masked:
                        pieces += [(it, h, m * BLK, HALF, HALF), (it, h, m * BLK + HALF, HALF, BLK)]
                    else:
                        pieces += [(it, h, m * BLK, BLK, BLK)]

        def scores(x):
            (n, qi, pj), h, at, wide, keys = pieces[x]
            cols = slice(at, at + wide)
            s = _dot(k[n, pj, h, :keys, :], qt[qi, h, :, cols], 1, 0)
            if masked:
                iota = lambda axis: lax.broadcasted_iota(jnp.int32, (keys, wide), axis)
                s = jnp.where(iota(1) + (at % BLK) >= iota(0), s, HIDDEN)
            sb[x % SB, :keys, :wide] = s
            old = top[qi, h, :, cols]
            new = jnp.maximum(old, s.max(axis=0, keepdims=True))
            top[qi, h, :, cols] = new
            return new, jnp.exp2((old - new) * e)

        def values(x, new, keep):
            (n, qi, pj), h, at, wide, keys = pieces[x]
            cols = slice(at, at + wide)
            part = None
            for k0 in range(0, keys, KS):
                p = jnp.exp2((sb[x % SB, k0 : k0 + KS, :wide] - new) * e).astype(jnp.bfloat16)
                more = _dot(vt[n, pj, h, :, k0 : k0 + KS], p, 1, 0)
                part = more if part is None else part + more
            acc[qi, h, :, cols] = acc[qi, h, :, cols] * keep + part

        ready = [scores(x) for x in range(AHEAD)]
        for x in range(len(pieces)):
            if x + AHEAD < len(pieces):
                ready.append(scores(x + AHEAD))
            values(x, *ready[x])

    def group_of(p):
        r = lax.div(p, 2)
        return jnp.where(r == 0, 0, jnp.where(r == 3, 3, 1 + _xor1(lax.rem(p, 2))))

    def slot_of(g, u):
        return jnp.where(g == 0, u, jnp.where(g == 3, 6 + _xor1(u), 2 + 2 * u + _xor1(jnp.maximum(g - 1, 0))))

    def last_group(i):
        out = i32(0)
        for j in range(N):
            out = jnp.maximum(out, jnp.where(i32(j) <= i, group_of(_xor(d, i32(j))), 0))
        return out

    def result_copy(src, dst, dev, at):
        return pltpu.make_async_remote_copy(res.at[src], res.at[dst], s_o.at[at], osem.at[dst], device_id={"sp": dev}, device_id_type=MESH)

    def finish(qi, g):
        second = qi >= 6
        slot = jnp.where(second, qi - 6, qi)

        last = last_group(_xor(d, slot))

        @pl.when(jnp.where(second & (last == 3), 4, last) == g)
        def _():
            to = jnp.where(slot == 0, qi, jnp.where(second, N, N + slot))
            for h in range(2):
                for n in range(2):
                    cols = slice(n * BLK, (n + 1) * BLK)
                    total = acc[qi, h, HEAD : HEAD + 1, cols]
                    o = (acc[qi, h, :HEAD, cols] * (1 / total)).T
                    res[to, :, (2 * h + n) * HEAD : (2 * h + n + 1) * HEAD] = o.astype(jnp.bfloat16)

            @pl.when(slot != 0)
            def _():
                result_copy(to, qi, _xor(d, slot), to - N).start()

    def wo_load(p):
        rows = pl.ds(pl.multiple_of(_xor(d, jnp.asarray(p, jnp.int32)) * QW, QW), QW)
        return pltpu.make_async_copy(wo_hbm.at[rows, :], abuf.at[p], wo_sem.at[p])

    def x_load(h):
        return pltpu.make_async_copy(x_hbm.at[:, h * 1024 : (h + 1) * 1024], w.at[0, h * BLK : (h + 1) * BLK, :], x_sem.at[h])

    def group(g, _):
        @pl.when((g == 1) | (g == 2))
        def _():
            zz = g - 1
            ps, px = 2 + _xor1(zz), 4 + _xor1(zz)
            to_y(zz).wait_recv()
            relay_x(zz).start()
            forward(ps).start()
            to_x(zz).wait_recv()
            relay_y(zz).start()
            forward(px).start()

        def chip(p):
            return lax.div(_xor(d, p), 2)

        tail = g == 4

        def arrive(x, _):
            half, u = lax.div(x, 2), lax.rem(x, 2)
            n = jnp.where(tail, 1, half)
            p = slot_of(jnp.where(tail, 3, g), u)

            for m in range(2):

                @pl.when((g == 0) & (x == 2 * m))
                def _():
                    for c in w_loads[3 * m : 3 * m + 3]:
                        c.wait()

            @pl.when((g == 3) & (n == 0))
            def _():
                relay_x(u).wait_recv()
                relay_y(u).wait_recv()
                forward(p).start()

            @pl.when((p != 0) & (n == 0))
            def _():
                part(0, p, nz * HALF, HALF, sib, s_sib.at[0], sibsem.at[p]).wait_recv()

            @pl.when(jnp.where(n == 0, (g < 3) | (d >= 2), ((g < 3) | (tail & (half == 0))) & (chip(p) <= lax.div(d, 2))))
            def _():
                project(n, p, jnp.where(n == 0, jnp.minimum(p, 5), 6 + jnp.minimum(p, 1)), jnp.where(n == 0, g < 3, g == 0))

            return _

        lax.fori_loop(0, 4, arrive, None)
        p0, p1 = slot_of(g, i32(0)), slot_of(g, i32(1))

        @pl.when(g == 3)
        def _():
            sib_a.wait_send()
            sib_b.wait_send()
            for zz in range(2):
                to_y(i32(zz)).wait_send()
                to_x(i32(zz)).wait_send()
                relay_x(i32(zz)).wait_send()
                relay_y(i32(zz)).wait_send()
            for p in range(2, 6):
                forward(i32(p)).wait_send()
            for p in range(6):
                wo_load(p).start()
            for h in range(2):
                x_load(h).start()

        @pl.when(tail)
        def _():
            for p in (6, 7):
                forward(i32(p)).wait_send()
                wo_load(p).start()

        b0, b1 = _xor(d, p0), _xor(d, p1)
        hi, lo = jnp.where(b0 > b1, p0, p1), jnp.where(b0 > b1, p1, p0)
        first = g == 0
        old = jnp.where(tail, 0, 2 * g)

        def pair(x, _):
            t = jnp.maximum(old - 1 - x, 0)
            told = slot_of(lax.div(t, 2), lax.rem(t, 2))
            is_old = x < old
            newy = jnp.where(tail, slot_of(3, x), jnp.where(x == old, p0, p1))
            ups = [_xor(d, told) > _xor(d, p) for p in (p0, p1)]
            qs = [jnp.where(first, o, jnp.where(is_old, jnp.where(up, told, p), m)) for o, up, p, m in zip((hi, 6 + hi), ups, (p0, p1), (6, 7))]
            ks = [jnp.where(first, lo, jnp.where(is_old, jnp.where(up, p, told), newy)) for up, p in zip(ups, (p0, p1))]
            sets = [jnp.where(first, o, jnp.where(is_old, 0, 1)) for o in (0, 1)]
            seen = (chip(newy) < lax.div(d, 2)).astype(jnp.int32)
            wanted = jnp.where(is_old, jnp.maximum(ups[0].astype(jnp.int32), (g < 3).astype(jnp.int32)), jnp.maximum(seen, first.astype(jnp.int32)))

            @pl.when(wanted == 1)
            def _():
                attend([(sets[0], qs[0], ks[0]), (sets[1], qs[1], ks[1])], False)

            @pl.when(is_old)
            def _():
                finish(told, g)

            return _

        lax.fori_loop(0, old + jnp.where(first, 1, jnp.where(g == 3, 0, 2)), pair, None)

        @pl.when((g == 1) | (g == 2))
        def _():
            attend([(0, hi, lo)], False)

        def diagonal(n, _):
            attend([(n, jnp.where(n == 0, p, 6 + u), p) for u, p in enumerate((p0, p1))], True)
            return _

        lax.fori_loop(0, jnp.where(first, 2, jnp.where(g >= 3, 0, 1)), diagonal, None)

        def close(x, _):
            qi = jnp.where(x < 2, jnp.where(x == 0, p0, p1), 4 + x)

            @pl.when((x >= 2) | (g < 3))
            def _():
                finish(qi, g)

            return _

        lax.fori_loop(0, 4, close, None)
        return _

    lax.fori_loop(0, 5, group, None)

    def output(sets, start, end):
        for p in sets:
            wo_load(p).wait()
            if not (isinstance(p, int) and p in (0, 6)):
                result_copy(0, p, sib, 0).wait_recv()

        def tile(t, _):
            cols = pl.ds(pl.multiple_of(t * TILE, TILE), TILE)
            y = None
            for p in sets:
                more = _dot(res[p], abuf[p, :, cols], 1, 0)
                y = more if y is None else y + more
            if not start:
                y = y + yacc[:, cols]
            if not end:
                yacc[:, cols] = y
            else:
                half, at = lax.div(t, 4), pl.ds(pl.multiple_of(lax.rem(t, 4) * TILE, TILE), TILE)
                rows = pl.ds(pl.multiple_of(half * BLK, BLK), BLK)
                w[1, rows, at] = (w[0, rows, at].astype(jnp.float32) + y).astype(jnp.bfloat16)
                y_store(t).start()
            return _

        lax.fori_loop(0, DM // TILE, tile, None)

    def y_store(t):
        half, at = lax.div(t, 4), pl.ds(pl.multiple_of(lax.rem(t, 4) * TILE, TILE), TILE)
        rows = pl.ds(pl.multiple_of(half * BLK, BLK), BLK)
        return pltpu.make_async_copy(w.at[1, rows, at], columns(y_hbm, t, TILE), y_sem.at[t])

    last_chip = d >= N - 2

    @pl.when(last_chip)
    def _():
        for h in range(2):
            x_load(h).wait()
        output((0, 6, 1, 7, 2, 3, 4, 5), True, True)

    @pl.when(jnp.logical_not(last_chip))
    def _():
        output((0, 6, 1, 7), True, False)
        for h in range(2):
            x_load(h).wait()
        near = jnp.where(lax.div(d, 2) == 2, 4, 2)
        output((near, near + 1), False, False)
        output((6 - near, 7 - near), False, True)

    for t in range(DM // TILE):
        y_store(i32(t)).wait()
    for at in range(6):
        result_copy(0, 1, sib, at).wait_send()


def _tables():
    freq = float(THETA) ** (-np.arange(HEAD // 2, dtype=np.float64) / (HEAD // 2))
    freq = np.concatenate([freq, freq])
    loc = np.arange(BLK, dtype=np.float64)[:, None] * freq
    base = (np.arange(N, dtype=np.float64) * BLK)[:, None] * freq
    return (np.stack([np.cos(loc), np.sin(loc)]).astype(np.float32),
            np.concatenate([np.cos(base), np.sin(base)]).astype(np.float32))


def solution(mesh):
    loc, base = _tables()

    def step(x, gain, wq, wk, wv, wo):
        dma, any_, vmem = pltpu.SemaphoreType.DMA, pl.BlockSpec(memory_space=pl.ANY), pl.BlockSpec(memory_space=pltpu.VMEM)
        return pl.pallas_call(
            _mega,
            out_shape=jax.ShapeDtypeStruct((BLK, DM), jnp.bfloat16),
            in_specs=[any_, vmem, any_, any_, any_, any_, vmem, vmem],
            out_specs=any_,
            scratch_shapes=[
                pltpu.VMEM((N, BLK, DM), jnp.bfloat16),
                pltpu.VMEM((2, DM, QW + 2 * KW), jnp.bfloat16),
                pltpu.VMEM((N, 2, HEAD, 2 * BLK), jnp.bfloat16),
                pltpu.VMEM((2, N, 2, BLK, HEAD), jnp.bfloat16),
                pltpu.VMEM((2, N, 2, ROWS_V, BLK), jnp.bfloat16),
                pltpu.VMEM((N, 2, ROWS_V, 2 * BLK), jnp.float32),
                pltpu.VMEM((N, 2, 1, 2 * BLK), jnp.float32),
                pltpu.VMEM((N + 6, BLK, QW), jnp.bfloat16),
                pltpu.VMEM((SB, BLK, BLK), jnp.float32),
                pltpu.VMEM((BLK, DM), jnp.float32),
                dma((4,)), dma((2, 3)), dma((N,)), dma((N,)), dma((2,)), dma((2,)),
                dma((2,)), dma((2, 2)), dma((2, 2)), dma((N,)), dma((6,)), dma((N,)), dma((N,)), dma((N,)),
            ],
            compiler_params=pltpu.CompilerParams(collective_id=0, has_side_effects=True, vmem_limit_bytes=67043328),
            cost_estimate=pl.CostEstimate(flops=6 * 10**10, transcendentals=4 * 10**7, bytes_accessed=64 * 2**20),
        )(x, gain, wq, wk, wv, wo, jnp.asarray(loc), jnp.asarray(base))

    tokens, whole = P(("dp", "sp"), None), P(None, None)
    return jax.shard_map(step, mesh=mesh, in_specs=(tokens, P(None), whole, whole, whole, whole), out_specs=tokens, check_vma=False)
```

```python
import jax
import jax.numpy as jnp
import numpy as np
from jax import lax
from jax.experimental import pallas as pl
from jax.experimental.pallas import tpu as pltpu
from jax.sharding import PartitionSpec as P

MESH = pl.DeviceIdType.MESH
NEG = -1e30
HIDDEN = 2 * NEG
LOG2E = 1.4426950408889634
HEAD = 128
THETA = 10000
N = 8
BLK = 512
HALF = BLK // 2
QUARTER = BLK // 4
DM = 2048
QW = 512
KW = 256
ROWS_V = 144
AHEAD = 2
SB = AHEAD + 1
KS = 256
TILE = 256


def _dot(a, b, ca, cb):
    return lax.dot_general(a, b, (((ca,), (cb,)), ((), ())), preferred_element_type=jnp.float32)


def _xor(a, b):
    out = 0
    for w in (4, 2, 1):
        p, q = (a >= w).astype(jnp.int32), (b >= w).astype(jnp.int32)
        a, b = a - w * p, b - w * q
        out = out + w * (p + q - 2 * p * q)
    return out


def _mega(x_hbm, gain_ref, wq_hbm, wk_hbm, wv_hbm, wo_hbm, loc_ref, base_ref, y_hbm,
          abuf, w, qt, k, vt, acc, top, res, sb, yacc,
          x_sem, w_sem, dsem, sibsem, qasem, qbsem, s_sib, s_dir, s_rel, s_fwd, s_o, osem, wo_sem, y_sem):
    i32 = lambda v: jnp.asarray(v, jnp.int32)
    d = lax.axis_index("sp").astype(jnp.int32)
    z = lax.rem(d, 2)
    nz = 1 - z
    sib, ynb, xnb = (_xor(d, i32(m)) for m in (1, 2, 4))
    e = HEAD**-0.5 * LOG2E

    def columns(ref, s, width):
        return ref.at[:, pl.ds(pl.multiple_of(s * width, width), width)]

    x_loads = [pltpu.make_async_copy(x_hbm.at[:, c * QW : (c + 1) * QW], res.at[N + c], x_sem.at[c]) for c in range(DM // QW)]
    w_loads = [
        pltpu.make_async_copy(columns(src, _xor(d, i32(6 * n)), width), w.at[n, :, at : at + width], w_sem.at[n, c])
        for n in range(2)
        for c, (src, at, width) in enumerate(((wq_hbm, 0, QW), (wk_hbm, QW, KW), (wv_hbm, QW + KW, KW)))
    ]
    for c in x_loads + w_loads[:3]:
        c.start()
    barrier = pltpu.get_barrier_semaphore()
    for m in range(1, N):
        pl.semaphore_signal(barrier, inc=1, device_id={"sp": _xor(d, i32(m))}, device_id_type=MESH)

    for c in x_loads:
        c.wait()
    gain = gain_ref[...].astype(jnp.float32).reshape(1, DM)
    STEP = 64

    def norm(r, _):
        rows = pl.ds(pl.multiple_of(r * STEP, STEP), STEP)
        wide = jnp.concatenate([res[N + c, rows, :].astype(jnp.float32) for c in range(DM // QW)], axis=1)
        scale = lax.rsqrt(jnp.mean(wide * wide, -1, keepdims=True) + 1e-6)
        abuf[0, rows, :] = (wide * scale * gain).astype(jnp.bfloat16)
        return _

    lax.fori_loop(0, BLK // STEP, norm, None)
    pl.semaphore_wait(barrier, N - 1)

    def _xor1(zz):
        return jnp.where(zz == z, 0, 1)

    def part(src, dst, at, rows, dev, ssem, rsem):
        here = pl.ds(pl.multiple_of(at, QUARTER), rows)
        return pltpu.make_async_remote_copy(abuf.at[src, here], abuf.at[dst, here], ssem, rsem, device_id={"sp": dev}, device_id_type=MESH)

    sib_a = part(0, 1, nz * HALF, HALF, sib, s_sib.at[0], dsem.at[1])
    sib_b = part(0, 1, z * HALF, HALF, sib, s_sib.at[1], sibsem.at[1])

    def to_y(zz):
        return part(_xor1(zz), 2 + _xor1(zz), z * HALF, HALF, ynb, s_dir.at[zz, 0], dsem.at[2 + _xor1(zz)])

    def to_x(zz):
        return part(_xor1(zz), 4 + _xor1(zz), z * HALF, HALF, xnb, s_dir.at[zz, 1], dsem.at[4 + _xor1(zz)])

    def relay_x(zz):
        return part(2 + _xor1(zz), 6 + _xor1(zz), z * HALF, QUARTER, xnb, s_rel.at[zz, 0], qasem.at[_xor1(zz)])

    def relay_y(zz):
        return part(4 + _xor1(zz), 6 + _xor1(zz), z * HALF + QUARTER, QUARTER, ynb, s_rel.at[zz, 1], qbsem.at[_xor1(zz)])

    def forward(p):
        return part(p, _xor(p, i32(1)), z * HALF, HALF, sib, s_fwd.at[p], sibsem.at[_xor(p, i32(1))])

    sib_a.start()

    @pl.when(z == 0)
    def _():
        to_y(i32(0)).start()
        to_x(i32(0)).start()

    sib_b.start()
    sib_a.wait_recv()

    @pl.when(z == 1)
    def _():
        to_y(i32(0)).start()
        to_x(i32(0)).start()

    to_y(i32(1)).start()
    to_x(i32(1)).start()
    for c in w_loads[3:]:
        c.start()
    ones = jnp.ones((ROWS_V - HEAD, BLK), jnp.bfloat16)
    lane = lax.broadcasted_iota(jnp.int32, (BLK, HEAD), 1)

    def project(n, p, qi, with_q):
        s = _xor(d, p)
        cb, sb_ = base_ref[pl.ds(s, 1), :], base_ref[pl.ds(N + s, 1), :]
        cl, sl = loc_ref[0], loc_ref[1]
        cos = cb * cl - sb_ * sl
        sin = sb_ * cl + cb * sl
        sin = jnp.where(lane < HEAD // 2, -sin, sin)

        def turn(t):
            t = t.astype(jnp.bfloat16).astype(jnp.float32)
            return t * cos + pltpu.roll(t, HEAD // 2, 1) * sin

        def piece(c):
            y = _dot(abuf[p], w[n, :, c * 256 : (c + 1) * 256], 1, 0)
            return y[:, :HEAD], y[:, HEAD:]

        @pl.when(with_q)
        def _():
            for c in range(2):
                for m, t in enumerate(piece(c)):
                    qt[qi, c, :, m * BLK : (m + 1) * BLK] = turn(t).T.astype(jnp.bfloat16)
            top[qi] = jnp.full((2, 1, 2 * BLK), NEG, jnp.float32)
            acc[qi] = jnp.zeros((2, ROWS_V, 2 * BLK), jnp.float32)

        for m, t in enumerate(piece(2)):
            k[n, p, m] = turn(t).astype(jnp.bfloat16)
        for m, t in enumerate(piece(3)):
            vt[n, p, m, :HEAD, :] = t.T.astype(jnp.bfloat16)
            vt[n, p, m, HEAD:, :] = ones

    def attend(items, masked):
        pieces = []
        for it in items:
            for h in range(2):
                for m in range(2):
                    if masked:
                        pieces += [(it, h, m * BLK, HALF, HALF), (it, h, m * BLK + HALF, HALF, BLK)]
                    else:
                        pieces += [(it, h, m * BLK, BLK, BLK)]

        def scores(x):
            (n, qi, pj), h, at, wide, keys = pieces[x]
            cols = slice(at, at + wide)
            s = _dot(k[n, pj, h, :keys, :], qt[qi, h, :, cols], 1, 0)
            if masked:
                iota = lambda axis: lax.broadcasted_iota(jnp.int32, (keys, wide), axis)
                s = jnp.where(iota(1) + (at % BLK) >= iota(0), s, HIDDEN)
            sb[x % SB, :keys, :wide] = s
            old = top[qi, h, :, cols]
            new = jnp.maximum(old, s.max(axis=0, keepdims=True))
            top[qi, h, :, cols] = new
            return new, jnp.exp2((old - new) * e)

        def values(x, new, keep):
            (n, qi, pj), h, at, wide, keys = pieces[x]
            cols = slice(at, at + wide)
            part = None
            for k0 in range(0, keys, KS):
                p = jnp.exp2((sb[x % SB, k0 : k0 + KS, :wide] - new) * e).astype(jnp.bfloat16)
                more = _dot(vt[n, pj, h, :, k0 : k0 + KS], p, 1, 0)
                part = more if part is None else part + more
            acc[qi, h, :, cols] = acc[qi, h, :, cols] * keep + part

        ready = [scores(x) for x in range(AHEAD)]
        for x in range(len(pieces)):
            if x + AHEAD < len(pieces):
                ready.append(scores(x + AHEAD))
            values(x, *ready[x])

    def slot_of(g, u):
        return jnp.where(g == 0, u, jnp.where(g == 3, 6 + _xor1(u), 2 + 2 * u + _xor1(jnp.maximum(g - 1, 0))))

    own_chip = lax.div(d, 2)
    chip_y = own_chip + 1 - 2 * lax.rem(own_chip, 2)
    chip_x = own_chip + 2 - 4 * lax.div(own_chip, 2)

    def last_group(i):
        c = lax.div(i, 2)
        beside = jnp.where((chip_y == c) | (chip_x == c), 1 + lax.rem(i, 2), 0)
        return jnp.where(3 - own_chip <= c, 3, jnp.where((chip_y < c) | (chip_x < c), 2, beside))

    def result_copy(src, dst, dev, at):
        return pltpu.make_async_remote_copy(res.at[src], res.at[dst], s_o.at[at], osem.at[dst], device_id={"sp": dev}, device_id_type=MESH)

    def finish(qi, g):
        second = qi >= 6
        slot = jnp.where(second, qi - 6, qi)

        last = last_group(_xor(d, slot))

        @pl.when(jnp.where(second & (last == 3), 4, last) == g)
        def _():
            to = jnp.where(slot == 0, qi, jnp.where(second, N, N + slot))
            for h in range(2):
                for n in range(2):
                    cols = slice(n * BLK, (n + 1) * BLK)
                    total = acc[qi, h, HEAD : HEAD + 1, cols]
                    o = (acc[qi, h, :HEAD, cols] * (1 / total)).T
                    res[to, :, (2 * h + n) * HEAD : (2 * h + n + 1) * HEAD] = o.astype(jnp.bfloat16)

            @pl.when(slot != 0)
            def _():
                result_copy(to, qi, _xor(d, slot), to - N).start()

    def wo_load(p):
        rows = pl.ds(pl.multiple_of(_xor(d, jnp.asarray(p, jnp.int32)) * QW, QW), QW)
        return pltpu.make_async_copy(wo_hbm.at[rows, :], abuf.at[p], wo_sem.at[p])

    def x_load(h):
        return pltpu.make_async_copy(x_hbm.at[:, h * 1024 : (h + 1) * 1024], w.at[0, h * BLK : (h + 1) * BLK, :], x_sem.at[h])

    def group(g, _):
        @pl.when((g == 1) | (g == 2))
        def _():
            zz = g - 1
            ps, px = 2 + _xor1(zz), 4 + _xor1(zz)
            to_y(zz).wait_recv()
            relay_x(zz).start()
            forward(ps).start()
            to_x(zz).wait_recv()
            relay_y(zz).start()
            forward(px).start()

        def chip(p):
            return lax.div(_xor(d, p), 2)

        tail = g == 4

        def arrive(x, _):
            half, u = lax.div(x, 2), lax.rem(x, 2)
            n = jnp.where(tail, 1, half)
            p = slot_of(jnp.where(tail, 3, g), u)

            for m in range(2):

                @pl.when((g == 0) & (x == 2 * m))
                def _():
                    for c in w_loads[3 * m : 3 * m + 3]:
                        c.wait()

            @pl.when((g == 3) & (n == 0))
            def _():
                relay_x(u).wait_recv()
                relay_y(u).wait_recv()
                forward(p).start()

            @pl.when((p != 0) & (n == 0))
            def _():
                part(0, p, nz * HALF, HALF, sib, s_sib.at[0], sibsem.at[p]).wait_recv()

            @pl.when(jnp.where(n == 0, (g < 3) | (d >= 2), ((g < 3) | (tail & (half == 0))) & (chip(p) <= lax.div(d, 2))))
            def _():
                project(n, p, jnp.where(n == 0, jnp.minimum(p, 5), 6 + jnp.minimum(p, 1)), jnp.where(n == 0, g < 3, g == 0))

            return _

        lax.fori_loop(0, 4, arrive, None)
        p0, p1 = slot_of(g, i32(0)), slot_of(g, i32(1))

        @pl.when(g == 3)
        def _():
            sib_a.wait_send()
            sib_b.wait_send()
            for zz in range(2):
                to_y(i32(zz)).wait_send()
                to_x(i32(zz)).wait_send()
                relay_x(i32(zz)).wait_send()
                relay_y(i32(zz)).wait_send()
            for p in range(2, 6):
                forward(i32(p)).wait_send()
            for p in range(6):
                wo_load(p).start()
            for h in range(2):
                x_load(h).start()

        @pl.when(tail)
        def _():
            for p in (6, 7):
                forward(i32(p)).wait_send()
                wo_load(p).start()

        b0, b1 = _xor(d, p0), _xor(d, p1)
        hi, lo = jnp.where(b0 > b1, p0, p1), jnp.where(b0 > b1, p1, p0)
        first = g == 0
        old = jnp.where(tail, 0, 2 * g)

        def pair(x, _):
            t = jnp.maximum(old - 1 - x, 0)
            told = slot_of(lax.div(t, 2), lax.rem(t, 2))
            is_old = x < old
            newy = jnp.where(tail, slot_of(3, x), jnp.where(x == old, p0, p1))
            ups = [_xor(d, told) > _xor(d, p) for p in (p0, p1)]
            qs = [jnp.where(first, o, jnp.where(is_old, jnp.where(up, told, p), m)) for o, up, p, m in zip((hi, 6 + hi), ups, (p0, p1), (6, 7))]
            ks = [jnp.where(first, lo, jnp.where(is_old, jnp.where(up, p, told), newy)) for up, p in zip(ups, (p0, p1))]
            sets = [jnp.where(first, o, jnp.where(is_old, 0, 1)) for o in (0, 1)]
            seen = (chip(newy) < lax.div(d, 2)).astype(jnp.int32)
            wanted = jnp.where(is_old, jnp.maximum(ups[0].astype(jnp.int32), (g < 3).astype(jnp.int32)), jnp.maximum(seen, first.astype(jnp.int32)))

            @pl.when(wanted == 1)
            def _():
                attend([(sets[0], qs[0], ks[0]), (sets[1], qs[1], ks[1])], False)

            @pl.when(is_old)
            def _():
                finish(told, g)

            return _

        lax.fori_loop(0, old + jnp.where(first, 1, jnp.where(g == 3, 0, 2)), pair, None)

        @pl.when((g == 1) | (g == 2))
        def _():
            attend([(0, hi, lo)], False)

        def diagonal(n, _):
            attend([(n, jnp.where(n == 0, p, 6 + u), p) for u, p in enumerate((p0, p1))], True)
            return _

        lax.fori_loop(0, jnp.where(first, 2, jnp.where(g >= 3, 0, 1)), diagonal, None)

        def close(x, _):
            qi = jnp.where(x < 2, jnp.where(x == 0, p0, p1), 4 + x)

            @pl.when((x >= 2) | (g < 3))
            def _():
                finish(qi, g)

            return _

        lax.fori_loop(0, 4, close, None)
        return _

    lax.fori_loop(0, 5, group, None)

    def output(sets, start, end):
        for p in sets:
            wo_load(p).wait()
            if not (isinstance(p, int) and p in (0, 6)):
                result_copy(0, p, sib, 0).wait_recv()

        def tile(t, _):
            cols = pl.ds(pl.multiple_of(t * TILE, TILE), TILE)
            y = None
            for p in sets:
                more = _dot(res[p], abuf[p, :, cols], 1, 0)
                y = more if y is None else y + more
            if not start:
                y = y + yacc[:, cols]
            if not end:
                yacc[:, cols] = y
            else:
                half, at = lax.div(t, 4), pl.ds(pl.multiple_of(lax.rem(t, 4) * TILE, TILE), TILE)
                rows = pl.ds(pl.multiple_of(half * BLK, BLK), BLK)
                w[1, rows, at] = (w[0, rows, at].astype(jnp.float32) + y).astype(jnp.bfloat16)
                y_store(t).start()
            return _

        lax.fori_loop(0, DM // TILE, tile, None)

    def y_store(t):
        half, at = lax.div(t, 4), pl.ds(pl.multiple_of(lax.rem(t, 4) * TILE, TILE), TILE)
        rows = pl.ds(pl.multiple_of(half * BLK, BLK), BLK)
        return pltpu.make_async_copy(w.at[1, rows, at], columns(y_hbm, t, TILE), y_sem.at[t])

    last_chip = d >= N - 2

    @pl.when(last_chip)
    def _():
        for h in range(2):
            x_load(h).wait()
        output((0, 6, 1, 7, 2, 3, 4, 5), True, True)

    @pl.when(jnp.logical_not(last_chip))
    def _():
        output((0, 6, 1, 7), True, False)
        for h in range(2):
            x_load(h).wait()
        near = jnp.where(lax.div(d, 2) == 2, 4, 2)
        output((near, near + 1), False, False)
        output((6 - near, 7 - near), False, True)

    for t in range(DM // TILE):
        y_store(i32(t)).wait()
    for at in range(6):
        result_copy(0, 1, sib, at).wait_send()


def _tables():
    freq = float(THETA) ** (-np.arange(HEAD // 2, dtype=np.float64) / (HEAD // 2))
    freq = np.concatenate([freq, freq])
    loc = np.arange(BLK, dtype=np.float64)[:, None] * freq
    base = (np.arange(N, dtype=np.float64) * BLK)[:, None] * freq
    return (np.stack([np.cos(loc), np.sin(loc)]).astype(np.float32),
            np.concatenate([np.cos(base), np.sin(base)]).astype(np.float32))


def solution(mesh):
    loc, base = _tables()

    def step(x, gain, wq, wk, wv, wo):
        dma, any_, vmem = pltpu.SemaphoreType.DMA, pl.BlockSpec(memory_space=pl.ANY), pl.BlockSpec(memory_space=pltpu.VMEM)
        return pl.pallas_call(
            _mega,
            out_shape=jax.ShapeDtypeStruct((BLK, DM), jnp.bfloat16),
            in_specs=[any_, vmem, any_, any_, any_, any_, vmem, vmem],
            out_specs=any_,
            scratch_shapes=[
                pltpu.VMEM((N, BLK, DM), jnp.bfloat16),
                pltpu.VMEM((2, DM, QW + 2 * KW), jnp.bfloat16),
                pltpu.VMEM((N, 2, HEAD, 2 * BLK), jnp.bfloat16),
                pltpu.VMEM((2, N, 2, BLK, HEAD), jnp.bfloat16),
                pltpu.VMEM((2, N, 2, ROWS_V, BLK), jnp.bfloat16),
                pltpu.VMEM((N, 2, ROWS_V, 2 * BLK), jnp.float32),
                pltpu.VMEM((N, 2, 1, 2 * BLK), jnp.float32),
                pltpu.VMEM((N + 6, BLK, QW), jnp.bfloat16),
                pltpu.VMEM((SB, BLK, BLK), jnp.float32),
                pltpu.VMEM((BLK, DM), jnp.float32),
                dma((4,)), dma((2, 3)), dma((N,)), dma((N,)), dma((2,)), dma((2,)),
                dma((2,)), dma((2, 2)), dma((2, 2)), dma((N,)), dma((6,)), dma((N,)), dma((N,)), dma((N,)),
            ],
            compiler_params=pltpu.CompilerParams(collective_id=0, has_side_effects=True, vmem_limit_bytes=67043328),
            cost_estimate=pl.CostEstimate(flops=6 * 10**10, transcendentals=4 * 10**7, bytes_accessed=64 * 2**20),
        )(x, gain, wq, wk, wv, wo, jnp.asarray(loc), jnp.asarray(base))

    tokens, whole = P(("dp", "sp"), None), P(None, None)
    return jax.shard_map(step, mesh=mesh, in_specs=(tokens, P(None), whole, whole, whole, whole), out_specs=tokens, check_vma=False)
```

```python
import jax
import jax.numpy as jnp
import numpy as np
from jax import lax
from jax.experimental import pallas as pl
from jax.experimental.pallas import tpu as pltpu
from jax.sharding import PartitionSpec as P

MESH = pl.DeviceIdType.MESH
NEG = -1e30
HIDDEN = 2 * NEG
LOG2E = 1.4426950408889634
HEAD = 128
THETA = 10000
N = 8
BLK = 512
HALF = BLK // 2
QUARTER = BLK // 4
DM = 2048
QW = 512
KW = 256
ROWS_V = 144
AHEAD = 2
SB = AHEAD + 1
KS = 256
TILE = 256


def _dot(a, b, ca, cb):
    return lax.dot_general(a, b, (((ca,), (cb,)), ((), ())), preferred_element_type=jnp.float32)


def _xor(a, b):
    out = 0
    for w in (4, 2, 1):
        p, q = (a >= w).astype(jnp.int32), (b >= w).astype(jnp.int32)
        a, b = a - w * p, b - w * q
        out = out + w * (p + q - 2 * p * q)
    return out


def _mega(x_hbm, gain_ref, wq_hbm, wk_hbm, wv_hbm, wo_hbm, loc_ref, base_ref, y_hbm,
          abuf, w, qt, k, vt, acc, top, res, sb, yacc,
          x_sem, w_sem, dsem, sibsem, qasem, qbsem, s_sib, s_dir, s_rel, s_fwd, s_o, osem, wo_sem, y_sem):
    i32 = lambda v: jnp.asarray(v, jnp.int32)
    d = lax.axis_index("sp").astype(jnp.int32)
    z = lax.rem(d, 2)
    nz = 1 - z
    sib, ynb, xnb = (_xor(d, i32(m)) for m in (1, 2, 4))
    e = HEAD**-0.5 * LOG2E

    def columns(ref, s, width):
        return ref.at[:, pl.ds(pl.multiple_of(s * width, width), width)]

    x_loads = [pltpu.make_async_copy(x_hbm.at[:, c * QW : (c + 1) * QW], res.at[N + c], x_sem.at[c]) for c in range(DM // QW)]
    w_loads = [
        pltpu.make_async_copy(columns(src, _xor(d, i32(6 * n)), width), w.at[n, :, at : at + width], w_sem.at[n, c])
        for n in range(2)
        for c, (src, at, width) in enumerate(((wq_hbm, 0, QW), (wk_hbm, QW, KW), (wv_hbm, QW + KW, KW)))
    ]
    for c in x_loads + w_loads[:3]:
        c.start()
    barrier = pltpu.get_barrier_semaphore()
    for m in range(1, N):
        pl.semaphore_signal(barrier, inc=1, device_id={"sp": _xor(d, i32(m))}, device_id_type=MESH)

    for c in x_loads:
        c.wait()
    gain = gain_ref[...].astype(jnp.float32).reshape(1, DM)
    STEP = 64

    def norm(r, _):
        rows = pl.ds(pl.multiple_of(r * STEP, STEP), STEP)
        wide = jnp.concatenate([res[N + c, rows, :].astype(jnp.float32) for c in range(DM // QW)], axis=1)
        scale = lax.rsqrt(jnp.mean(wide * wide, -1, keepdims=True) + 1e-6)
        abuf[0, rows, :] = (wide * scale * gain).astype(jnp.bfloat16)
        return _

    per = HALF // STEP
    lax.fori_loop(nz * per, nz * per + per, norm, None)
    pl.semaphore_wait(barrier, N - 1)

    def _xor1(zz):
        return jnp.where(zz == z, 0, 1)

    def part(src, dst, at, rows, dev, ssem, rsem):
        here = pl.ds(pl.multiple_of(at, QUARTER), rows)
        return pltpu.make_async_remote_copy(abuf.at[src, here], abuf.at[dst, here], ssem, rsem, device_id={"sp": dev}, device_id_type=MESH)

    sib_a = part(0, 1, nz * HALF, HALF, sib, s_sib.at[0], dsem.at[1])
    sib_b = part(0, 1, z * HALF, HALF, sib, s_sib.at[1], sibsem.at[1])

    def to_y(zz):
        return part(_xor1(zz), 2 + _xor1(zz), z * HALF, HALF, ynb, s_dir.at[zz, 0], dsem.at[2 + _xor1(zz)])

    def to_x(zz):
        return part(_xor1(zz), 4 + _xor1(zz), z * HALF, HALF, xnb, s_dir.at[zz, 1], dsem.at[4 + _xor1(zz)])

    def relay_x(zz):
        return part(2 + _xor1(zz), 6 + _xor1(zz), z * HALF, QUARTER, xnb, s_rel.at[zz, 0], qasem.at[_xor1(zz)])

    def relay_y(zz):
        return part(4 + _xor1(zz), 6 + _xor1(zz), z * HALF + QUARTER, QUARTER, ynb, s_rel.at[zz, 1], qbsem.at[_xor1(zz)])

    def forward(p):
        return part(p, _xor(p, i32(1)), z * HALF, HALF, sib, s_fwd.at[p], sibsem.at[_xor(p, i32(1))])

    sib_a.start()
    lax.fori_loop(z * per, z * per + per, norm, None)

    @pl.when(z == 0)
    def _():
        to_y(i32(0)).start()
        to_x(i32(0)).start()

    sib_b.start()
    sib_a.wait_recv()

    @pl.when(z == 1)
    def _():
        to_y(i32(0)).start()
        to_x(i32(0)).start()

    to_y(i32(1)).start()
    to_x(i32(1)).start()
    for c in w_loads[3:]:
        c.start()
    ones = jnp.ones((ROWS_V - HEAD, BLK), jnp.bfloat16)
    lane = lax.broadcasted_iota(jnp.int32, (BLK, HEAD), 1)

    def project(n, p, qi, with_q):
        s = _xor(d, p)
        cb, sb_ = base_ref[pl.ds(s, 1), :], base_ref[pl.ds(N + s, 1), :]
        cl, sl = loc_ref[0], loc_ref[1]
        cos = cb * cl - sb_ * sl
        sin = sb_ * cl + cb * sl
        sin = jnp.where(lane < HEAD // 2, -sin, sin)

        def turn(t):
            t = t.astype(jnp.bfloat16).astype(jnp.float32)
            return t * cos + pltpu.roll(t, HEAD // 2, 1) * sin

        def piece(c):
            y = _dot(abuf[p], w[n, :, c * 256 : (c + 1) * 256], 1, 0)
            return y[:, :HEAD], y[:, HEAD:]

        @pl.when(with_q)
        def _():
            for c in range(2):
                for m, t in enumerate(piece(c)):
                    qt[qi, c, :, m * BLK : (m + 1) * BLK] = turn(t).T.astype(jnp.bfloat16)
            top[qi] = jnp.full((2, 1, 2 * BLK), NEG, jnp.float32)
            acc[qi] = jnp.zeros((2, ROWS_V, 2 * BLK), jnp.float32)

        for m, t in enumerate(piece(2)):
            k[n, p, m] = turn(t).astype(jnp.bfloat16)
        for m, t in enumerate(piece(3)):
            vt[n, p, m, :HEAD, :] = t.T.astype(jnp.bfloat16)
            vt[n, p, m, HEAD:, :] = ones

    def attend(items, masked):
        pieces = []
        for it in items:
            for h in range(2):
                for m in range(2):
                    if masked:
                        pieces += [(it, h, m * BLK, HALF, HALF), (it, h, m * BLK + HALF, HALF, BLK)]
                    else:
                        pieces += [(it, h, m * BLK, BLK, BLK)]

        def scores(x):
            (n, qi, pj), h, at, wide, keys = pieces[x]
            cols = slice(at, at + wide)
            s = _dot(k[n, pj, h, :keys, :], qt[qi, h, :, cols], 1, 0)
            if masked:
                iota = lambda axis: lax.broadcasted_iota(jnp.int32, (keys, wide), axis)
                s = jnp.where(iota(1) + (at % BLK) >= iota(0), s, HIDDEN)
            sb[x % SB, :keys, :wide] = s
            old = top[qi, h, :, cols]
            new = jnp.maximum(old, s.max(axis=0, keepdims=True))
            top[qi, h, :, cols] = new
            return new, jnp.exp2((old - new) * e)

        def values(x, new, keep):
            (n, qi, pj), h, at, wide, keys = pieces[x]
            cols = slice(at, at + wide)
            part = None
            for k0 in range(0, keys, KS):
                p = jnp.exp2((sb[x % SB, k0 : k0 + KS, :wide] - new) * e).astype(jnp.bfloat16)
                more = _dot(vt[n, pj, h, :, k0 : k0 + KS], p, 1, 0)
                part = more if part is None else part + more
            acc[qi, h, :, cols] = acc[qi, h, :, cols] * keep + part

        ready = [scores(x) for x in range(AHEAD)]
        for x in range(len(pieces)):
            if x + AHEAD < len(pieces):
                ready.append(scores(x + AHEAD))
            values(x, *ready[x])

    def slot_of(g, u):
        return jnp.where(g == 0, u, jnp.where(g == 3, 6 + _xor1(u), 2 + 2 * u + _xor1(jnp.maximum(g - 1, 0))))

    own_chip = lax.div(d, 2)
    chip_y = own_chip + 1 - 2 * lax.rem(own_chip, 2)
    chip_x = own_chip + 2 - 4 * lax.div(own_chip, 2)

    def last_group(i):
        c = lax.div(i, 2)
        beside = jnp.where((chip_y == c) | (chip_x == c), 1 + lax.rem(i, 2), 0)
        return jnp.where(3 - own_chip <= c, 3, jnp.where((chip_y < c) | (chip_x < c), 2, beside))

    def result_copy(src, dst, dev, at):
        return pltpu.make_async_remote_copy(res.at[src], res.at[dst], s_o.at[at], osem.at[dst], device_id={"sp": dev}, device_id_type=MESH)

    def finish(qi, g):
        second = qi >= 6
        slot = jnp.where(second, qi - 6, qi)

        last = last_group(_xor(d, slot))

        @pl.when(jnp.where(second & (last == 3), 4, last) == g)
        def _():
            to = jnp.where(slot == 0, qi, jnp.where(second, N, N + slot))
            for h in range(2):
                for n in range(2):
                    cols = slice(n * BLK, (n + 1) * BLK)
                    total = acc[qi, h, HEAD : HEAD + 1, cols]
                    o = (acc[qi, h, :HEAD, cols] * (1 / total)).T
                    res[to, :, (2 * h + n) * HEAD : (2 * h + n + 1) * HEAD] = o.astype(jnp.bfloat16)

            @pl.when(slot != 0)
            def _():
                result_copy(to, qi, _xor(d, slot), to - N).start()

    def wo_load(p):
        rows = pl.ds(pl.multiple_of(_xor(d, jnp.asarray(p, jnp.int32)) * QW, QW), QW)
        return pltpu.make_async_copy(wo_hbm.at[rows, :], abuf.at[p], wo_sem.at[p])

    def x_load(h):
        return pltpu.make_async_copy(x_hbm.at[:, h * 1024 : (h + 1) * 1024], w.at[0, h * BLK : (h + 1) * BLK, :], x_sem.at[h])

    def group(g, _):
        @pl.when((g == 1) | (g == 2))
        def _():
            zz = g - 1
            ps, px = 2 + _xor1(zz), 4 + _xor1(zz)
            to_y(zz).wait_recv()
            relay_x(zz).start()
            forward(ps).start()
            to_x(zz).wait_recv()
            relay_y(zz).start()
            forward(px).start()

        def chip(p):
            return lax.div(_xor(d, p), 2)

        tail = g == 4

        def arrive(x, _):
            half, u = lax.div(x, 2), lax.rem(x, 2)
            n = jnp.where(tail, 1, half)
            p = slot_of(jnp.where(tail, 3, g), u)

            for m in range(2):

                @pl.when((g == 0) & (x == 2 * m))
                def _():
                    for c in w_loads[3 * m : 3 * m + 3]:
                        c.wait()

            @pl.when((g == 3) & (n == 0))
            def _():
                relay_x(u).wait_recv()
                relay_y(u).wait_recv()
                forward(p).start()

            @pl.when((p != 0) & (n == 0))
            def _():
                part(0, p, nz * HALF, HALF, sib, s_sib.at[0], sibsem.at[p]).wait_recv()

            @pl.when(jnp.where(n == 0, (g < 3) | (d >= 2), ((g < 3) | (tail & (half == 0))) & (chip(p) <= lax.div(d, 2))))
            def _():
                project(n, p, jnp.where(n == 0, jnp.minimum(p, 5), 6 + jnp.minimum(p, 1)), jnp.where(n == 0, g < 3, g == 0))

            return _

        lax.fori_loop(0, 4, arrive, None)
        p0, p1 = slot_of(g, i32(0)), slot_of(g, i32(1))

        @pl.when(g == 3)
        def _():
            sib_a.wait_send()
            sib_b.wait_send()
            for zz in range(2):
                to_y(i32(zz)).wait_send()
                to_x(i32(zz)).wait_send()
                relay_x(i32(zz)).wait_send()
                relay_y(i32(zz)).wait_send()
            for p in range(2, 6):
                forward(i32(p)).wait_send()
            for p in range(6):
                wo_load(p).start()
            for h in range(2):
                x_load(h).start()

        @pl.when(tail)
        def _():
            for p in (6, 7):
                forward(i32(p)).wait_send()
                wo_load(p).start()

        b0, b1 = _xor(d, p0), _xor(d, p1)
        hi, lo = jnp.where(b0 > b1, p0, p1), jnp.where(b0 > b1, p1, p0)
        first = g == 0
        old = jnp.where(tail, 0, 2 * g)

        def pair(x, _):
            t = jnp.maximum(old - 1 - x, 0)
            told = slot_of(lax.div(t, 2), lax.rem(t, 2))
            is_old = x < old
            newy = jnp.where(tail, slot_of(3, x), jnp.where(x == old, p0, p1))
            ups = [_xor(d, told) > _xor(d, p) for p in (p0, p1)]
            qs = [jnp.where(first, o, jnp.where(is_old, jnp.where(up, told, p), m)) for o, up, p, m in zip((hi, 6 + hi), ups, (p0, p1), (6, 7))]
            ks = [jnp.where(first, lo, jnp.where(is_old, jnp.where(up, p, told), newy)) for up, p in zip(ups, (p0, p1))]
            sets = [jnp.where(first, o, jnp.where(is_old, 0, 1)) for o in (0, 1)]
            seen = (chip(newy) < lax.div(d, 2)).astype(jnp.int32)
            wanted = jnp.where(is_old, jnp.maximum(ups[0].astype(jnp.int32), (g < 3).astype(jnp.int32)), jnp.maximum(seen, first.astype(jnp.int32)))

            @pl.when(wanted == 1)
            def _():
                attend([(sets[0], qs[0], ks[0]), (sets[1], qs[1], ks[1])], False)

            @pl.when(is_old)
            def _():
                finish(told, g)

            return _

        lax.fori_loop(0, old + jnp.where(first, 1, jnp.where(g == 3, 0, 2)), pair, None)

        @pl.when((g == 1) | (g == 2))
        def _():
            attend([(0, hi, lo)], False)

        def diagonal(n, _):
            attend([(n, jnp.where(n == 0, p, 6 + u), p) for u, p in enumerate((p0, p1))], True)
            return _

        lax.fori_loop(0, jnp.where(first, 2, jnp.where(g >= 3, 0, 1)), diagonal, None)

        def close(x, _):
            qi = jnp.where(x < 2, jnp.where(x == 0, p0, p1), 4 + x)

            @pl.when((x >= 2) | (g < 3))
            def _():
                finish(qi, g)

            return _

        lax.fori_loop(0, 4, close, None)
        return _

    lax.fori_loop(0, 5, group, None)

    def output(sets, start, end):
        for p in sets:
            wo_load(p).wait()
            if not (isinstance(p, int) and p in (0, 6)):
                result_copy(0, p, sib, 0).wait_recv()

        def tile(t, _):
            cols = pl.ds(pl.multiple_of(t * TILE, TILE), TILE)
            y = None
            for p in sets:
                more = _dot(res[p], abuf[p, :, cols], 1, 0)
                y = more if y is None else y + more
            if not start:
                y = y + yacc[:, cols]
            if not end:
                yacc[:, cols] = y
            else:
                half, at = lax.div(t, 4), pl.ds(pl.multiple_of(lax.rem(t, 4) * TILE, TILE), TILE)
                rows = pl.ds(pl.multiple_of(half * BLK, BLK), BLK)
                w[1, rows, at] = (w[0, rows, at].astype(jnp.float32) + y).astype(jnp.bfloat16)
                y_store(t).start()
            return _

        lax.fori_loop(0, DM // TILE, tile, None)

    def y_store(t):
        half, at = lax.div(t, 4), pl.ds(pl.multiple_of(lax.rem(t, 4) * TILE, TILE), TILE)
        rows = pl.ds(pl.multiple_of(half * BLK, BLK), BLK)
        return pltpu.make_async_copy(w.at[1, rows, at], columns(y_hbm, t, TILE), y_sem.at[t])

    last_chip = d >= N - 2

    @pl.when(last_chip)
    def _():
        for h in range(2):
            x_load(h).wait()
        output((0, 6, 1, 7, 2, 3, 4, 5), True, True)

    @pl.when(jnp.logical_not(last_chip))
    def _():
        output((0, 6, 1, 7), True, False)
        for h in range(2):
            x_load(h).wait()
        near = jnp.where(lax.div(d, 2) == 2, 4, 2)
        output((near, near + 1), False, False)
        output((6 - near, 7 - near), False, True)

    for t in range(DM // TILE):
        y_store(i32(t)).wait()
    for at in range(6):
        result_copy(0, 1, sib, at).wait_send()


def _tables():
    freq = float(THETA) ** (-np.arange(HEAD // 2, dtype=np.float64) / (HEAD // 2))
    freq = np.concatenate([freq, freq])
    loc = np.arange(BLK, dtype=np.float64)[:, None] * freq
    base = (np.arange(N, dtype=np.float64) * BLK)[:, None] * freq
    return (np.stack([np.cos(loc), np.sin(loc)]).astype(np.float32),
            np.concatenate([np.cos(base), np.sin(base)]).astype(np.float32))


def solution(mesh):
    loc, base = _tables()

    def step(x, gain, wq, wk, wv, wo):
        dma, any_, vmem = pltpu.SemaphoreType.DMA, pl.BlockSpec(memory_space=pl.ANY), pl.BlockSpec(memory_space=pltpu.VMEM)
        return pl.pallas_call(
            _mega,
            out_shape=jax.ShapeDtypeStruct((BLK, DM), jnp.bfloat16),
            in_specs=[any_, vmem, any_, any_, any_, any_, vmem, vmem],
            out_specs=any_,
            scratch_shapes=[
                pltpu.VMEM((N, BLK, DM), jnp.bfloat16),
                pltpu.VMEM((2, DM, QW + 2 * KW), jnp.bfloat16),
                pltpu.VMEM((N, 2, HEAD, 2 * BLK), jnp.bfloat16),
                pltpu.VMEM((2, N, 2, BLK, HEAD), jnp.bfloat16),
                pltpu.VMEM((2, N, 2, ROWS_V, BLK), jnp.bfloat16),
                pltpu.VMEM((N, 2, ROWS_V, 2 * BLK), jnp.float32),
                pltpu.VMEM((N, 2, 1, 2 * BLK), jnp.float32),
                pltpu.VMEM((N + 6, BLK, QW), jnp.bfloat16),
                pltpu.VMEM((SB, BLK, BLK), jnp.float32),
                pltpu.VMEM((BLK, DM), jnp.float32),
                dma((4,)), dma((2, 3)), dma((N,)), dma((N,)), dma((2,)), dma((2,)),
                dma((2,)), dma((2, 2)), dma((2, 2)), dma((N,)), dma((6,)), dma((N,)), dma((N,)), dma((N,)),
            ],
            compiler_params=pltpu.CompilerParams(collective_id=0, has_side_effects=True, vmem_limit_bytes=67043328),
            cost_estimate=pl.CostEstimate(flops=6 * 10**10, transcendentals=4 * 10**7, bytes_accessed=64 * 2**20),
        )(x, gain, wq, wk, wv, wo, jnp.asarray(loc), jnp.asarray(base))

    tokens, whole = P(("dp", "sp"), None), P(None, None)
    return jax.shard_map(step, mesh=mesh, in_specs=(tokens, P(None), whole, whole, whole, whole), out_specs=tokens, check_vma=False)
```
